32 devices in a mesh: seq: 16 (over z, x, core), head: 2 (over y).
Axes of the slice: x: 2, y: 2, z: 4, core: 2. Of those that a mesh axis runs over, the one named last changes fastest.
Arguments:
- hidden: bfloat16 [4608, 8192], P('seq'), may hold values from -6 to 6
- norm_gain: bfloat16 [8192], replicated, may hold values from 0.099609375 to 1.8984375
- w_query: bfloat16 [8192, 1024], P('seq', 'head'), may hold values from -0.125 to 0.125
- w_key: bfloat16 [8192, 256], P('seq', 'head'), may hold values from -0.125 to 0.125
- w_value: bfloat16 [8192, 256], P('seq', 'head'), may hold values from -0.0625 to 0.0625
- bias_query: bfloat16 [1024], P('head'), may hold values from -3 to 3
- bias_key: bfloat16 [256], P('head'), may hold values from -200 to 200
- bias_value: bfloat16 [256], P('head'), may hold values from -3 to 3
- w_out: bfloat16 [1024, 8192], P('head', 'seq'), may hold values from -0.1875 to 0.1875
Outputs:
- attn_out: bfloat16 [4608, 8192], P(('seq', 'head'))
The draws below stay inside these ranges and needn't reach their ends.
All inputs are finite; a program needn't handle non-finite values.
Results may differ from the reference program's by a relative error of at most 0.014.
The reference program's roundings to bfloat16 on the way count: a program that leaves them out, or rounds other values in their place, can miss the bound.
Values may be sent and summed in bfloat16 or wider, within the bound.
No kernel may reach another device: no remote copies, remote signals or barrier semaphores. Data moves between devices by JAX's collectives and lax.ppermute only.
A program may use at most 192 MiB of HBM per device.

```python
import jax
import jax.numpy as jnp
from jax import lax

D = 8192
HEAD_DIM = 128
QPG = 4
KV_HEADS = 2
LENGTH = 4608


def draw_bias_key(key, part):
    count = KV_HEADS * HEAD_DIM
    base = jax.random.normal(key, (count,), jnp.float32)
    return jnp.clip(0.5 * base, -3.0, 3.0).astype(jnp.bfloat16)


def steps_of(own_key, extent, split, least, high):
    gain = 1.0
    for position, shards_of in split:
        heights = jax.random.uniform(jax.random.fold_in(jax.random.fold_in(own_key, 6), position), (shards_of,), jnp.float32, least / len(split), high / len(split))
        gain = gain * jnp.repeat(jnp.exp(heights), extent[position] // shards_of).reshape((-1,) + (1,) * (len(extent) - 1 - position))
    return gain


def noise(own_key, dims, deviation, limit, split=(), kind=jnp.bfloat16):
    values = deviation * jax.random.normal(own_key, dims, jnp.float32)
    if split:
        values = values * steps_of(own_key, dims, split, -0.22, 0.18)
    return jnp.clip(values, -limit, limit).astype(kind)


def setup_inputs(seed: int = 0) -> dict:
    key_of = jax.random.split(jax.random.key(seed), 10)
    hidden = noise(key_of[0], (LENGTH, D), 1.0, 6.0, ((0, 16),))
    norm_gain = jnp.clip(1.0 + 0.18 * jax.random.normal(key_of[1], (D,), jnp.float32), 0.099609375, 1.8984375).astype(jnp.bfloat16)
    w_query = noise(key_of[2], (D, KV_HEADS * QPG * HEAD_DIM), (D // 4) ** -0.5, 0.125, ((0, 16), (1, 2)))
    w_key = noise(key_of[3], (D, KV_HEADS * HEAD_DIM), (D // 4) ** -0.5, 0.125, ((0, 16), (1, 2)))
    w_value = noise(key_of[4], (D, KV_HEADS * HEAD_DIM), D ** -0.5, 0.0625, ((0, 16), (1, 2)))
    bias_query = noise(key_of[5], (KV_HEADS * QPG * HEAD_DIM,), 0.5, 3.0, ((0, 2),))
    bias_key = draw_bias_key(jax.random.fold_in(key_of[9], 71), 0)
    bias_value = noise(key_of[7], (KV_HEADS * HEAD_DIM,), 0.5, 3.0, ((0, 2),))
    w_out = noise(key_of[8], (KV_HEADS * QPG * HEAD_DIM, D), (KV_HEADS * QPG * HEAD_DIM) ** -0.5, 0.1875, ((0, 2), (1, 16)))
    return dict(hidden=hidden, norm_gain=norm_gain, w_query=w_query, w_key=w_key, w_value=w_value, bias_query=bias_query, bias_key=bias_key, bias_value=bias_value, w_out=w_out)


ROPE_BASE = 1000000.0
EPSILON = 1e-06

def rotary(values, positions):
    half = values.shape[-1] // 2
    freq = ROPE_BASE ** (-2.0 * jnp.arange(half, dtype=jnp.float32) / values.shape[-1])
    angles = positions.astype(jnp.float32)[:, None, None] * freq[None, None, :]
    cosine = jnp.cos(angles)
    sine = jnp.sin(angles)
    first = values[..., :half]
    second = values[..., half:]
    return jnp.concatenate([first * cosine - second * sine, second * cosine + first * sine], axis=-1)

def reference(hidden, norm_gain, w_query, w_key, w_value, bias_query, bias_key, bias_value, w_out):
    length = hidden.shape[0]
    widened = hidden.astype(jnp.float32)
    inverse = lax.rsqrt(lax.optimization_barrier(jnp.mean(widened * widened, axis=-1, keepdims=True)) + EPSILON)
    normed = (widened * inverse * norm_gain.astype(jnp.float32)).astype(jnp.bfloat16)
    positions = jnp.arange(length, dtype=jnp.int32)
    query = jnp.dot(normed, w_query, preferred_element_type=jnp.float32) + bias_query.astype(jnp.float32)
    keys = jnp.dot(normed, w_key, preferred_element_type=jnp.float32) + bias_key.astype(jnp.float32)
    values = jnp.dot(normed, w_value, preferred_element_type=jnp.float32) + bias_value.astype(jnp.float32)
    query = rotary(query.reshape(length, KV_HEADS * QPG, HEAD_DIM), positions).astype(jnp.bfloat16)
    keys = rotary(keys.reshape(length, KV_HEADS, HEAD_DIM), positions).astype(jnp.bfloat16)
    values = values.reshape(length, KV_HEADS, HEAD_DIM).astype(jnp.bfloat16)
    query_groups = query.reshape(length, KV_HEADS, QPG, HEAD_DIM).transpose(1, 2, 0, 3)
    key_groups = keys.transpose(1, 0, 2)
    value_groups = values.transpose(1, 0, 2)
    causal = positions[:, None] >= positions[None, :]
    out_groups = w_out.reshape(KV_HEADS, QPG * HEAD_DIM, w_out.shape[1])

    def attend(carry, group):
        group_query, group_key, group_value, group_out = group
        scores = jnp.einsum('hqd,kd->hqk', group_query.astype(jnp.float32), group_key.astype(jnp.float32)) * HEAD_DIM ** (-0.5)
        scores = jnp.where(causal[None], scores, -jnp.inf)
        highest = lax.optimization_barrier(jnp.max(scores, axis=-1, keepdims=True))
        probs = jnp.exp(scores - highest)
        total = lax.optimization_barrier(jnp.sum(probs, axis=-1, keepdims=True))
        rounded = lax.optimization_barrier(probs.astype(jnp.bfloat16))
        mixed = jnp.einsum('hqk,kd->hqd', rounded.astype(jnp.float32), group_value.astype(jnp.float32))
        attended = (mixed / total).astype(jnp.bfloat16)
        attended = attended.transpose(1, 0, 2).reshape(length, QPG * HEAD_DIM)
        term = jnp.dot(attended, group_out, preferred_element_type=jnp.float32)
        term = lax.optimization_barrier(term.astype(jnp.bfloat16))
        return (carry + term.astype(jnp.float32), None)
    start = jnp.zeros((length, w_out.shape[1]), jnp.float32)
    summed, unused = lax.scan(attend, start, (query_groups, key_groups, value_groups, out_groups))
    return summed.astype(jnp.bfloat16)
```

```python
import functools

import jax
import jax.numpy as jnp
from jax import lax
from jax.experimental import pallas as pl
from jax.experimental.pallas import tpu as pltpu
from jax.sharding import PartitionSpec as P

HEAD_DIM = 128
ROPE_BASE = 1000000.0
EPSILON = 1e-06
LOG2E = 1.4426950408889634


VMEM = pl.BlockSpec(memory_space=pltpu.VMEM)
SMEM = pl.BlockSpec(memory_space=pltpu.SMEM)


def dot(a, b, dims=((1,), (0,))):
    return lax.dot_general(a, b, (dims, ((), ())), preferred_element_type=jnp.float32)


def ring_place(seq_size, shard):
    rows = seq_size // 4
    chip = shard // 2
    return jnp.where(chip % 2 == 0, chip // 2, 2 * rows - 1 - chip // 2)


def ring_chip(seq_size, place):
    rows = seq_size // 4
    if place < rows:
        return 2 * place
    return 2 * (2 * rows - 1 - place) + 1


def ring_perm(seq_size):
    chips = seq_size // 2
    pairs = []
    for place in range(chips):
        here = ring_chip(seq_size, place) * 2
        pairs.append((here, ring_chip(seq_size, (place + 1) % chips) * 2))
        pairs.append((here + 1, ring_chip(seq_size, (place - 1) % chips) * 2 + 1))
    return pairs


def slot_shards(seq_size, shard):
    chips = seq_size // 2
    rows = seq_size // 4
    place = ring_place(seq_size, shard)
    core = shard % 2
    out = []
    for which in (core, 1 - core):
        way = jnp.where(which == 0, -1, 1)
        for step in range(chips // 2 + 1):
            at = (place + way * step) % chips
            chip = jnp.where(at < rows, 2 * at, 2 * (2 * rows - 1 - at) + 1)
            out.append(chip * 2 + which)
            if 0 < step < chips // 2:
                out.append(chip * 2 + 1 - which)
    return jnp.stack(out).astype(jnp.int32)


def swap_core(value, seq_size):
    return lax.ppermute(value, "seq", [(s, s ^ 1) for s in range(seq_size)])


def swap_head(value):
    return lax.ppermute(value, "head", [(0, 1), (1, 0)])


def pass_on(value, seq_size):
    return lax.ppermute(value, "seq", ring_perm(seq_size))


def ring_gather(own, other, seq_size, name):
    half = seq_size // 4
    held = [own]
    first, second = own, other
    for step in range(1, half + 1):
        with jax.named_scope(f"{name}_a{step}"):
            first = pass_on(first, seq_size)
        held.append(first)
        if step < half:
            with jax.named_scope(f"{name}_b{step}"):
                second = pass_on(second, seq_size)
            held.append(second)
    return held


def norm_kernel(table, hidden, gain, mine, other):
    slots, rows, depth = mine.shape
    width = hidden.shape[1]
    squares = jnp.zeros((rows, 128), jnp.float32)
    for start in range(0, width, depth):
        part = hidden[:, start : start + depth].astype(jnp.float32)
        part = part * part
        for lane in range(0, depth, 128):
            squares = squares + part[:, lane : lane + 128]
    mean = jnp.sum(squares, axis=1, keepdims=True) * (1.0 / width)
    inverse = lax.rsqrt(mean + EPSILON)
    for slot in range(2 * slots):
        columns = pl.ds(pl.multiple_of(table[slot] * depth, depth), depth)
        value = hidden[:, columns].astype(jnp.float32) * inverse
        value = (value * gain[:, columns].astype(jnp.float32)).astype(jnp.bfloat16)
        if slot < slots:
            mine[slot] = value
        else:
            other[slot - slots] = value


def norm(table, hidden, gain, slots, depth):
    rows = hidden.shape[0]
    shape = jax.ShapeDtypeStruct((slots, rows, depth), jnp.bfloat16)
    return pl.pallas_call(
        norm_kernel,
        out_shape=(shape, shape),
        in_specs=[SMEM, VMEM, VMEM],
        out_specs=(VMEM, VMEM),
        cost_estimate=pl.CostEstimate(
            flops=4 * 10**9, bytes_accessed=4 * hidden.size, transcendentals=0
        ),
        name="norm",
    )(table, hidden, gain)


def project_kernel(slots, *refs):
    mine, other = refs[:2]
    weights = refs[2 : 2 + slots]
    keep, send = refs[2 + slots :]
    for source, target in ((other, send), (mine, keep)):
        total = dot(source[0], weights[0][...])
        for slot in range(1, slots):
            total = total + dot(source[slot], weights[slot][...])
        target[...] = total


def project(mine, other, weights, name):
    slots, rows, depth = mine.shape
    columns = weights[0].shape[1]
    shape = jax.ShapeDtypeStruct((rows, columns), jnp.float32)
    return pl.pallas_call(
        functools.partial(project_kernel, slots),
        out_shape=(shape, shape),
        in_specs=[VMEM] * (2 + slots),
        out_specs=(VMEM, VMEM),
        cost_estimate=pl.CostEstimate(
            flops=4 * slots * rows * depth * columns,
            bytes_accessed=4 * slots * rows * depth,
            transcendentals=0,
        ),
        name=name,
    )(mine, other, *weights)


def rotated(value, cosine, sine):
    return value * cosine + pltpu.roll(value, HEAD_DIM // 2, 1) * sine


def keys_values_kernel(keep, got, bias, cosine, sine, out):
    total = keep[...] + got[...] + bias[...]
    out[:, :HEAD_DIM] = rotated(total[:, :HEAD_DIM], cosine[...], sine[...]).astype(
        jnp.bfloat16
    )
    out[:, HEAD_DIM:] = total[:, HEAD_DIM:].astype(jnp.bfloat16)


def keys_values(keep, got, bias, cosine, sine):
    return pl.pallas_call(
        keys_values_kernel,
        out_shape=jax.ShapeDtypeStruct(keep.shape, jnp.bfloat16),
        in_specs=[VMEM] * 5,
        out_specs=VMEM,
        cost_estimate=pl.CostEstimate(
            flops=10**9, bytes_accessed=10 * keep.size, transcendentals=0
        ),
        name="keys_values",
    )(keep, got, bias, cosine, sine)


def attend_kernel(
    places, heads, table, keep, got, bias, cosine, sine, *refs
):
    sources = refs[: len(refs) - 5]
    out, query, highest, total, summed = refs[len(refs) - 5 :]
    rows = keep.shape[0]
    shard = table[0]
    for head in range(heads):
        columns = slice(head * HEAD_DIM, (head + 1) * HEAD_DIM)
        value = keep[:, columns] + got[:, columns] + bias[:, columns]
        query[head * rows : (head + 1) * rows] = rotated(
            value, cosine[...], sine[...]
        ).astype(jnp.bfloat16)
    factor = HEAD_DIM ** (-0.5) * LOG2E

    def update(slot, first):
        ref, at = places[slot]
        block = sources[ref]
        keys = block[at, :, :HEAD_DIM]
        values = block[at, :, HEAD_DIM:]
        for head in range(heads):
            span = slice(head * rows, (head + 1) * rows)
            scores = dot(query[span], keys, ((1,), (1,)))
            if first:
                row = lax.broadcasted_iota(jnp.int32, (rows, rows), 0)
                column = lax.broadcasted_iota(jnp.int32, (rows, rows), 1)
                scores = jnp.where(row >= column, scores, -jnp.inf)
            top = jnp.max(scores, axis=1, keepdims=True)
            if not first:
                top = jnp.maximum(top, highest[span])
            probs = jnp.exp2((scores - top) * factor)
            added = jnp.sum(probs, axis=1, keepdims=True)
            mixed = dot(probs.astype(jnp.bfloat16), values)
            if not first:
                scale = jnp.exp2((highest[span] - top) * factor)
                added = added + total[span] * scale
                mixed = mixed + summed[span] * scale
            highest[span] = top
            total[span] = added
            summed[span] = mixed

    update(0, True)
    for slot in range(1, len(places)):

        @pl.when(table[slot] < shard)
        def _(slot=slot):
            update(slot, False)

    for head in range(heads):
        span = slice(head * rows, (head + 1) * rows)
        out[:, head * HEAD_DIM : (head + 1) * HEAD_DIM] = (
            summed[span] / total[span]
        ).astype(jnp.bfloat16)


def attend(table, keep, got, bias, cosine, sine, sources, places):
    rows, columns = keep.shape
    heads = columns // HEAD_DIM
    work = 4 * len(places) * rows * rows * columns
    return pl.pallas_call(
        functools.partial(attend_kernel, places, heads),
        out_shape=jax.ShapeDtypeStruct((rows, columns), jnp.bfloat16),
        in_specs=[SMEM] + [VMEM] * (5 + len(sources)),
        out_specs=VMEM,
        scratch_shapes=[
            pltpu.VMEM((heads * rows, HEAD_DIM), jnp.bfloat16),
            pltpu.VMEM((heads * rows, 1), jnp.float32),
            pltpu.VMEM((heads * rows, 1), jnp.float32),
            pltpu.VMEM((heads * rows, HEAD_DIM), jnp.float32),
        ],
        cost_estimate=pl.CostEstimate(
            flops=4 * work, bytes_accessed=work // 1000, transcendentals=0
        ),
        name="attend",
    )(table, keep, got, bias, cosine, sine, *sources)


def out_kernel(pieces, place, mine, across, mine_other, across_other, *refs):
    weights = refs[:pieces]
    keep, send = refs[pieces:]
    rows = mine.shape[0] // 2
    half = place[0]
    near = pl.ds(pl.multiple_of(half * rows, 16), rows)
    far = pl.ds(pl.multiple_of((1 - half) * rows, 16), rows)
    for target, span in ((send, far), (keep, near)):
        for core, (left, right) in enumerate(
            ((mine, across), (mine_other, across_other))
        ):
            first = left[span, :]
            second = right[span, :]
            depth = first.shape[1]
            for piece in range(pieces):
                block = weights[piece]
                one = dot(first, block[:depth]).astype(jnp.bfloat16)
                two = dot(second, block[depth:]).astype(jnp.bfloat16)
                target[core, piece] = (
                    one.astype(jnp.float32) + two.astype(jnp.float32)
                ).astype(jnp.bfloat16)


def project_out(place, attended, weights, name):
    pieces = len(weights)
    rows, depth = attended[0].shape
    columns = weights[0].shape[1]
    shape = jax.ShapeDtypeStruct((2, pieces, rows // 2, columns), jnp.bfloat16)
    return pl.pallas_call(
        functools.partial(out_kernel, pieces),
        out_shape=(shape, shape),
        in_specs=[SMEM] + [VMEM] * (4 + pieces),
        out_specs=(VMEM, VMEM),
        cost_estimate=pl.CostEstimate(
            flops=8 * pieces * rows * depth * columns,
            bytes_accessed=8 * pieces * rows * columns,
            transcendentals=0,
        ),
        name=name,
    )(place, *attended, *weights)


def place_kernel(counts, slots, width, table, place, *refs):
    out = refs[-1]
    columns = out.shape[1] // (4 * slots)
    half = place[0]
    start = 0
    for index, count in enumerate(counts):
        keep, got, other = refs[3 * index : 3 * index + 3]
        for piece in range(count):
            here = table[start + piece] * width
            there = table[slots + start + piece] * width
            for value, base, side in (
                (keep[0, piece], here, half),
                (got[0, piece], here, 1 - half),
                (other[0, piece], there, half),
                (other[1, piece], there, 1 - half),
            ):
                at = pl.multiple_of(base + side * columns, columns)
                out[:, pl.ds(at, columns)] = value
        start += count


def place_all(table, place, parts, counts, slots, width):
    rows, columns = parts[0].shape[2:]
    return pl.pallas_call(
        functools.partial(place_kernel, counts, slots, width),
        out_shape=jax.ShapeDtypeStruct((rows, 4 * slots * columns), jnp.bfloat16),
        in_specs=[SMEM, SMEM] + [VMEM] * len(parts),
        out_specs=VMEM,
        name="place",
    )(table, place, *parts)


def fast(
    seq_size, hidden, norm_gain, w_query, w_key, w_value, bias_query, bias_key,
    bias_value, w_out,
):
    rows, width = hidden.shape
    depth = w_query.shape[0]
    slots = seq_size // 2
    half_chips = seq_size // 4
    shard = lax.axis_index("seq")
    side = lax.axis_index("head")
    table = slot_shards(seq_size, shard)
    place = jnp.reshape(side, (1,)).astype(jnp.int32)

    w_kv = jnp.concatenate([w_key, w_value], axis=1)
    with jax.named_scope("swap_kv"):
        w_kv_other = swap_core(w_kv, seq_size)
    kv_weights = ring_gather(w_kv, w_kv_other, seq_size, "ring_kv")
    mine, for_other = norm(table, hidden, norm_gain.reshape(1, width), slots, depth)
    with jax.named_scope("swap_normed"):
        other = swap_core(for_other, seq_size)

    positions = shard * rows + jnp.arange(rows, dtype=jnp.int32)
    half_dim = HEAD_DIM // 2
    freq = ROPE_BASE ** (-2.0 * jnp.arange(half_dim, dtype=jnp.float32) / HEAD_DIM)
    angles = positions.astype(jnp.float32)[:, None] * freq[None, :]
    cosine = jnp.cos(angles)
    sine = jnp.sin(angles)
    cosine = jnp.concatenate([cosine, cosine], axis=1)
    sine = jnp.concatenate([-sine, sine], axis=1)

    keep, send = project(mine, other, kv_weights, "project_kv")
    with jax.named_scope("swap_kv_sum"):
        got = swap_core(send, seq_size)
    bias_kv = jnp.concatenate([bias_key, bias_value]).astype(jnp.float32)[None]
    own_kv = keys_values(keep, got, bias_kv, cosine, sine)
    with jax.named_scope("swap_own_kv"):
        other_kv = swap_core(own_kv, seq_size)
    block = jnp.stack([own_kv, other_kv])
    blocks = [block]
    for step in range(1, half_chips + 1):
        with jax.named_scope(f"ring_tok{step}"):
            block = pass_on(block if step < half_chips else block[:1], seq_size)
        blocks.append(block)
    with jax.named_scope("swap_tok"):
        swapped = swap_core(jnp.concatenate(blocks[1:]), seq_size)
    sources = blocks + [swapped]
    places = [(0, 0)]
    for step in range(1, half_chips + 1):
        places.append((step, 0))
        if step < half_chips:
            places.append((step, 1))
    places.append((0, 1))
    places += [(half_chips + 1, at) for at in range(slots - 1)]

    with jax.named_scope("swap_q"):
        w_query_other = swap_core(w_query, seq_size)
    q_weights = ring_gather(w_query, w_query_other, seq_size, "ring_q")
    keep, send = project(mine, other, q_weights, "project_q")
    with jax.named_scope("swap_q_sum"):
        got = swap_core(send, seq_size)
    attended = attend(
        table, keep, got, bias_query.astype(jnp.float32)[None], cosine, sine,
        sources, places,
    )

    columns = w_out.shape[1] // 2
    near = lax.dynamic_slice_in_dim(w_out, side * columns, columns, 1)
    far = lax.dynamic_slice_in_dim(w_out, (1 - side) * columns, columns, 1)
    with jax.named_scope("swap_out_head"):
        far = swap_head(far)
    piece = jnp.concatenate([near, far])
    with jax.named_scope("swap_out"):
        piece_other = swap_core(piece, seq_size)
    out_weights = ring_gather(piece, piece_other, seq_size, "ring_out")

    with jax.named_scope("att_head"):
        across = swap_head(attended)
    with jax.named_scope("att_core"):
        both = swap_core(jnp.stack([attended, across]), seq_size)
    operands = (attended, across, both[0], both[1])
    counts = (slots - 3, 3)
    parts = []
    start = 0
    for index, count in enumerate(counts):
        keep, send = project_out(
            place, operands, out_weights[start : start + count], f"out{index}"
        )
        with jax.named_scope(f"out_head{index}"):
            got = swap_head(send)
        with jax.named_scope(f"out_core{index}"):
            theirs = swap_core(jnp.stack([keep[1], got[1]]), seq_size)
        parts += [keep, got, theirs]
        start += count
    return place_all(table, place, parts, counts, slots, w_out.shape[1])


def rotary(values, positions):
    half_dim = values.shape[-1] // 2
    freq = ROPE_BASE ** (-2.0 * jnp.arange(half_dim, dtype=jnp.float32) / values.shape[-1])
    angles = positions.astype(jnp.float32)[:, None, None] * freq[None, None, :]
    cosine = jnp.cos(angles)
    sine = jnp.sin(angles)
    first = values[..., :half_dim]
    second = values[..., half_dim:]
    return jnp.concatenate(
        [first * cosine - second * sine, second * cosine + first * sine], axis=-1
    )


def plain(hidden, norm_gain, w_query, w_key, w_value, bias_query, bias_key, bias_value, w_out):
    rows = hidden.shape[0]
    heads = w_query.shape[1] // HEAD_DIM
    positions = lax.axis_index("seq") * rows + jnp.arange(rows, dtype=jnp.int32)
    widened = hidden.astype(jnp.float32)
    inverse = lax.rsqrt(jnp.mean(widened * widened, axis=-1, keepdims=True) + EPSILON)
    normed = (widened * inverse * norm_gain.astype(jnp.float32)).astype(jnp.bfloat16)
    weights = jnp.concatenate([w_query, w_key, w_value], axis=1)
    biases = jnp.concatenate([bias_query, bias_key, bias_value]).astype(jnp.float32)
    weights = lax.all_gather(weights, "seq", axis=0, tiled=True)
    qkv = jnp.dot(normed, weights, preferred_element_type=jnp.float32) + biases
    query, keys, values = jnp.split(
        qkv, [heads * HEAD_DIM, (heads + 1) * HEAD_DIM], axis=1
    )
    query = rotary(query.reshape(rows, heads, HEAD_DIM), positions).astype(jnp.bfloat16)
    keys = rotary(keys.reshape(rows, 1, HEAD_DIM), positions).reshape(rows, HEAD_DIM)
    pair = jnp.concatenate([keys, values], axis=1).astype(jnp.bfloat16)
    pair = lax.all_gather(pair, "seq", axis=0, tiled=True)
    scores = jnp.einsum(
        "qhd,kd->hqk", query, pair[:, :HEAD_DIM], preferred_element_type=jnp.float32
    )
    allowed = positions[:, None] >= jnp.arange(pair.shape[0], dtype=jnp.int32)[None, :]
    scores = jnp.where(allowed[None], scores * HEAD_DIM ** (-0.5), -jnp.inf)
    probs = jnp.exp(scores - jnp.max(scores, axis=-1, keepdims=True))
    total = jnp.sum(probs, axis=-1, keepdims=True)
    mixed = jnp.einsum(
        "hqk,kd->hqd",
        probs.astype(jnp.bfloat16),
        pair[:, HEAD_DIM:],
        preferred_element_type=jnp.float32,
    )
    attended = (mixed / total).astype(jnp.bfloat16)
    attended = attended.transpose(1, 0, 2).reshape(rows, heads * HEAD_DIM)
    partial_out = jnp.dot(
        attended,
        lax.all_gather(w_out, "seq", axis=1, tiled=True),
        preferred_element_type=jnp.float32,
    )
    return lax.psum_scatter(
        partial_out.astype(jnp.bfloat16), "head", scatter_dimension=0, tiled=True
    )


def local(seq_size, head_size, *args):
    hidden, w_query, w_out = args[0], args[2], args[8]
    fits = (
        head_size == 2
        and seq_size % 4 == 0
        and seq_size >= 8
        and hidden.shape[0] % 32 == 0
        and w_query.shape[0] % 128 == 0
        and w_out.shape[1] % 256 == 0
    )
    if fits:
        return fast(seq_size, *args)
    return plain(*args)


def solution(mesh):
    in_specs = (
        P("seq", None),
        P(),
        P("seq", "head"),
        P("seq", "head"),
        P("seq", "head"),
        P("head"),
        P("head"),
        P("head"),
        P("head", "seq"),
    )
    out_specs = P(("seq", "head"), None)
    body = functools.partial(local, mesh.shape["seq"], mesh.shape["head"])
    return jax.shard_map(body, mesh=mesh, in_specs=in_specs, out_specs=out_specs, check_vma=False)
```

```python
import functools

import jax
import jax.numpy as jnp
from jax import lax
from jax.experimental import pallas as pl
from jax.experimental.pallas import tpu as pltpu
from jax.sharding import PartitionSpec as P

HEAD_DIM = 128
ROPE_BASE = 1000000.0
EPSILON = 1e-06
LOG2E = 1.4426950408889634


VMEM = pl.BlockSpec(memory_space=pltpu.VMEM)
SMEM = pl.BlockSpec(memory_space=pltpu.SMEM)
HBM = pl.BlockSpec(memory_space=pltpu.HBM)


GRANT = pltpu.CompilerParams(vmem_limit_bytes=28 << 20)


def estimate(microseconds):
    return pl.CostEstimate(
        flops=microseconds * 10**9, bytes_accessed=10**6, transcendentals=0
    )


def dot(a, b, dims=((1,), (0,))):
    return lax.dot_general(a, b, (dims, ((), ())), preferred_element_type=jnp.float32)


def ring_place(seq_size, shard):
    rows = seq_size // 4
    chip = shard // 2
    return jnp.where(chip % 2 == 0, chip // 2, 2 * rows - 1 - chip // 2)


def ring_chip(seq_size, place):
    rows = seq_size // 4
    if place < rows:
        return 2 * place
    return 2 * (2 * rows - 1 - place) + 1


def ring_perm(seq_size, turn):
    chips = seq_size // 2
    pairs = []
    for place in range(chips):
        here = ring_chip(seq_size, place) * 2
        pairs.append((here, ring_chip(seq_size, (place + turn) % chips) * 2))
        pairs.append((here + 1, ring_chip(seq_size, (place - turn) % chips) * 2 + 1))
    return pairs


def slot_shards(seq_size, shard, turn=1):
    chips = seq_size // 2
    rows = seq_size // 4
    place = ring_place(seq_size, shard)
    core = shard % 2
    out = []
    for which in (core, 1 - core):
        way = jnp.where(which == 0, -turn, turn)
        for step in range(chips // 2 + 1):
            at = (place + way * step) % chips
            chip = jnp.where(at < rows, 2 * at, 2 * (2 * rows - 1 - at) + 1)
            out.append(chip * 2 + which)
            if 0 < step < chips // 2:
                out.append(chip * 2 + 1 - which)
    return out


def swap_core(value, seq_size):
    return lax.ppermute(value, "seq", [(s, s ^ 1) for s in range(seq_size)])


def swap_head(value):
    return lax.ppermute(value, "head", [(0, 1), (1, 0)])


def swap_both(value, seq_size):
    pairs = [(i, (((i // 2) ^ 1) * 2) + (1 - i % 2)) for i in range(2 * seq_size)]
    return lax.ppermute(value, ("seq", "head"), pairs)


def pass_on(value, seq_size, turn):
    return lax.ppermute(value, "seq", ring_perm(seq_size, turn))


def ring_gather(own, other, seq_size, turn=1):
    half = seq_size // 4
    held = [own]
    first, second = own, other
    for step in range(1, half + 1):
        first = pass_on(first, seq_size, turn)
        held.append(first)
        if step < half:
            second = pass_on(second, seq_size, turn)
            held.append(second)
    return held


def norm_kernel(table, hidden, gain, mine, other):
    slots, rows, depth = mine.shape
    width = hidden.shape[1]

    def columns_of(index):
        return pl.ds(pl.multiple_of(index * depth, depth), depth)

    def square(index, squares):
        part = hidden[:, columns_of(index)].astype(jnp.float32)
        part = part * part
        for lane in range(0, depth, 128):
            squares = squares + part[:, lane : lane + 128]
        return squares

    squares = jnp.zeros((rows, 128), jnp.float32)
    squares = lax.fori_loop(0, width // depth, square, squares)
    mean = jnp.sum(squares, axis=1, keepdims=True) * (1.0 / width)
    inverse = lax.rsqrt(mean + EPSILON)
    for start, target in ((0, mine), (slots, other)):

        @pl.loop(0, slots)
        def _(slot, start=start, target=target):
            columns = columns_of(table[start + slot])
            value = hidden[:, columns].astype(jnp.float32) * inverse
            value = value * gain[:, columns].astype(jnp.float32)
            target[slot] = value.astype(jnp.bfloat16)


def norm(table, hidden, gain, slots, depth):
    rows = hidden.shape[0]
    shape = jax.ShapeDtypeStruct((slots, rows, depth), jnp.bfloat16)
    return pl.pallas_call(
        norm_kernel,
        out_shape=(shape, shape),
        in_specs=[SMEM, VMEM, VMEM],
        out_specs=(VMEM, VMEM),
        compiler_params=GRANT,
        cost_estimate=estimate(4),
        name="norm",
    )(table, hidden, gain)


def project_kernel(start, count, mine, other, *refs):
    weights = refs[:count]
    keep, send = refs[-2:]
    carried = refs[count:-2]
    for source, target, old in zip(
        (other, mine), (send, keep), carried[::-1] or (None, None)
    ):
        total = None if old is None else old[...]
        for slot in range(count):
            term = dot(source[start + slot], weights[slot][...])
            total = term if total is None else total + term
        target[...] = total


def project(mine, other, weights, start, carried):
    count = len(weights)
    shape = (mine.shape[1], weights[0].shape[1])
    shape = jax.ShapeDtypeStruct(shape, jnp.float32)
    return pl.pallas_call(
        functools.partial(project_kernel, start, count),
        out_shape=(shape, shape),
        in_specs=[VMEM] * (2 + count + len(carried)),
        out_specs=(VMEM, VMEM),
        compiler_params=GRANT,
        cost_estimate=estimate(4),
    )(mine, other, *weights, *carried)


def rotated(value, cosine, sine):
    return value * cosine + pltpu.roll(value, HEAD_DIM // 2, 1) * sine


def keys_values_kernel(keep, got, bias, cosine, sine, out):
    total = keep[...] + got[...] + bias[...]
    out[:, :HEAD_DIM] = rotated(total[:, :HEAD_DIM], cosine[...], sine[...]).astype(
        jnp.bfloat16
    )
    out[:, HEAD_DIM:] = total[:, HEAD_DIM:].astype(jnp.bfloat16)


def keys_values(keep, got, bias, cosine, sine):
    return pl.pallas_call(
        keys_values_kernel,
        out_shape=jax.ShapeDtypeStruct(keep.shape, jnp.bfloat16),
        in_specs=[VMEM] * 5,
        out_specs=VMEM,
        compiler_params=GRANT,
        cost_estimate=estimate(1),
        name="kv",
    )(keep, got, bias, cosine, sine)


def query_kernel(keep, got, bias, cosine, sine, out):
    parts = []
    for column in range(0, keep.shape[1], HEAD_DIM):
        span = slice(column, column + HEAD_DIM)
        value = keep[:, span] + got[:, span] + bias[:, span]
        parts.append(rotated(value, cosine[...], sine[...]))
    out[...] = jnp.concatenate(parts, axis=0).T.astype(jnp.bfloat16)


def queries(keep, got, bias, cosine, sine):
    rows, columns = keep.shape
    shape = (HEAD_DIM, rows * columns // HEAD_DIM)
    return pl.pallas_call(
        query_kernel,
        out_shape=jax.ShapeDtypeStruct(shape, jnp.bfloat16),
        in_specs=[VMEM] * 5,
        out_specs=VMEM,
        compiler_params=GRANT,
        cost_estimate=estimate(2),
        name="qs",
    )(keep, got, bias, cosine, sine)


def attend_kernel(first, count, offset, table, query, *refs):
    inputs = len(refs) - (7 if first else 8)
    carried = () if first else refs[inputs - 3 : inputs]
    sources = refs[: inputs - (0 if first else 3)]
    if first:
        high, weight, mixture = refs[inputs : inputs + 3]
        pairs, sems, even, odd = refs[inputs + 3 :]
    else:
        out = refs[inputs]
        pairs, sems, even, odd, high, weight, mixture = refs[inputs + 1 :]
    rows, _ = sources[0].shape[-2:]
    lanes = query.shape[1]
    shard = table[0]
    factor = HEAD_DIM ** (-0.5) * LOG2E

    def copy(slot, at):
        pltpu.make_async_copy(sources[slot], pairs.at[at], sems.at[at]).start()

    def wait(at):
        pltpu.make_async_copy(pairs.at[at], pairs.at[at], sems.at[at]).wait()

    start = 1 if first else 0
    if first:
        copy(0, 0)
    needed = jnp.int32(0)
    for slot in range(start, count):
        seen = table[offset + slot] < shard

        @pl.when(seen)
        def _(slot=slot, needed=needed):
            copy(slot, needed + start)

        needed = needed + seen.astype(jnp.int32)
    for new, old in zip((high, weight, mixture), carried):
        new[...] = old[...]

    def keys_of(at, size):
        return pairs[pl.ds(at, size), :, :HEAD_DIM].reshape(size * rows, HEAD_DIM)

    def values_of(at, size):
        return pairs[pl.ds(at, size), :, HEAD_DIM:].reshape(size * rows, HEAD_DIM).T

    def update(scores, values, fresh):
        top = jnp.max(scores, axis=0, keepdims=True)
        if not fresh:
            top = jnp.maximum(top, high[...])
        probs = jnp.exp2((scores - top) * factor)
        added = jnp.sum(probs, axis=0, keepdims=True)
        mixed = dot(values, probs.astype(jnp.bfloat16))
        if not fresh:
            scale = jnp.exp2((high[...] - top) * factor)
            added = added + weight[...] * scale
            mixed = mixed + mixture[...] * scale
        high[...] = top
        weight[...] = added
        mixture[...] = mixed

    if first:
        wait(0)
        scores = dot(keys_of(0, 1), query[...])
        row = lax.broadcasted_iota(jnp.int32, scores.shape, 0)
        lane = lax.rem(lax.broadcasted_iota(jnp.int32, (1, lanes), 1), rows)
        update(jnp.where(row <= lane, scores, -jnp.inf), values_of(0, 1), True)

    single = lax.rem(needed, 2)

    @pl.when(single == 1)
    def _():
        wait(start)
        update(dot(keys_of(start, 1), query[...]), values_of(start, 1), False)

    begin = start + single
    turns = needed // 2

    def arrive(turn):
        wait(begin + 2 * turn)
        wait(begin + 2 * turn + 1)

    def step(turn, here, there):
        @pl.when(turn + 1 < turns)
        def _():
            arrive(turn + 1)

        at = begin + 2 * jnp.minimum(turn + 1, turns - 1)
        there[...] = dot(keys_of(at, 2), query[...])
        update(here[...], values_of(begin + 2 * turn, 2), False)

    @pl.when(turns > 0)
    def _():
        arrive(0)
        even[...] = dot(keys_of(begin, 2), query[...])

        @pl.loop(0, (turns + 1) // 2)
        def _(index):
            step(2 * index, even, odd)

            @pl.when(2 * index + 1 < turns)
            def _():
                step(2 * index + 1, odd, even)

    if not first:
        value = (mixture[...] / weight[...]).T
        for head in range(lanes // rows):
            out[:, head * HEAD_DIM : (head + 1) * HEAD_DIM] = value[
                head * rows : (head + 1) * rows
            ].astype(jnp.bfloat16)


def attend(table, query, sources, offset, carried):
    count = len(sources)
    lanes = query.shape[1]
    rows = sources[0].shape[-2]
    first = not carried
    state = [
        ((1, lanes), jnp.float32),
        ((1, lanes), jnp.float32),
        ((HEAD_DIM, lanes), jnp.float32),
    ]
    if first:
        out_shape = tuple(jax.ShapeDtypeStruct(*one) for one in state)
        out_specs = (VMEM,) * 3
    else:
        out_shape = jax.ShapeDtypeStruct((rows, lanes // rows * HEAD_DIM), jnp.bfloat16)
        out_specs = VMEM
    scratch = [
        pltpu.VMEM((count, rows, 2 * HEAD_DIM), jnp.bfloat16),
        pltpu.SemaphoreType.DMA((count,)),
        pltpu.VMEM((2 * rows, lanes), jnp.float32),
        pltpu.VMEM((2 * rows, lanes), jnp.float32),
    ]
    if not first:
        scratch += [pltpu.VMEM(*one) for one in state]
    return pl.pallas_call(
        functools.partial(attend_kernel, first, count, offset),
        out_shape=out_shape,
        in_specs=[SMEM, VMEM] + [HBM] * len(sources) + [VMEM] * len(carried),
        out_specs=out_specs,
        scratch_shapes=scratch,
        compiler_params=GRANT,
        cost_estimate=estimate(8),
    )(table, query, *sources, *carried)


def out_kernel(pieces, place, mine, across, mine_other, across_other, *refs):
    weights = refs[:pieces]
    keep, keep_other, send, send_other, source, block, sems, weight_sems = refs[pieces:]
    rows = mine.shape[0] // 2
    depth = mine.shape[1]
    half = place[0]
    near = pl.ds(pl.multiple_of(half * rows, 16), rows)
    far = pl.ds(pl.multiple_of((1 - half) * rows, 16), rows)
    copies = []
    for group, (own, other) in enumerate(((mine, mine_other), (across, across_other))):
        for part, (ref, span) in enumerate(
            ((own, near), (other, near), (own, far), (other, far))
        ):
            copies.append(
                pltpu.make_async_copy(
                    ref.at[span],
                    source.at[group, pl.ds(part * rows, rows)],
                    sems.at[group, part],
                )
            )
    for copy in copies:
        copy.start()
    for piece in range(pieces):
        pltpu.make_async_copy(
            weights[piece], block.at[piece], weight_sems.at[piece]
        ).start()
    for copy in copies:
        copy.wait()

    @pl.loop(0, pieces)
    def _(piece):
        pltpu.make_async_copy(
            block.at[piece], block.at[piece], weight_sems.at[piece]
        ).wait()
        one = dot(source[0], block[piece, :depth]).astype(jnp.bfloat16)
        two = dot(source[1], block[piece, depth:]).astype(jnp.bfloat16)
        value = (one.astype(jnp.float32) + two.astype(jnp.float32)).astype(jnp.bfloat16)
        for part, target in enumerate((keep, keep_other, send, send_other)):
            target[piece] = value[part * rows : (part + 1) * rows]


def project_out(place, attended, weights):
    pieces = len(weights)
    rows, depth = attended[0].shape
    columns = weights[0].shape[1]
    shape = jax.ShapeDtypeStruct((pieces, rows // 2, columns), jnp.bfloat16)
    return pl.pallas_call(
        functools.partial(out_kernel, pieces),
        out_shape=(shape,) * 4,
        in_specs=[SMEM] + [HBM] * (4 + pieces),
        out_specs=(VMEM,) * 4,
        scratch_shapes=[
            pltpu.VMEM((2, 2 * rows, depth), jnp.bfloat16),
            pltpu.VMEM((pieces, 2 * depth, columns), jnp.bfloat16),
            pltpu.SemaphoreType.DMA((2, 4)),
            pltpu.SemaphoreType.DMA((pieces,)),
        ],
        compiler_params=GRANT,
        cost_estimate=estimate(3),
    )(place, *attended, *weights)


def place_kernel(start, slots, width, table, place, *refs):
    keep, got, other, across = refs[:4]
    out, sems = refs[-2:]
    pieces, _, columns = keep.shape
    half = place[0]
    copies = []
    for piece in range(pieces):
        here = table[start + piece] * width
        there = table[slots + start + piece] * width
        for index, (value, base, side) in enumerate(
            (
                (keep, here, half),
                (got, here, 1 - half),
                (other, there, half),
                (across, there, 1 - half),
            )
        ):
            at = pl.multiple_of(base + side * columns, columns)
            copies.append(
                pltpu.make_async_copy(
                    value.at[piece], out.at[:, pl.ds(at, columns)], sems.at[index, piece]
                )
            )
    for copy in copies:
        copy.start()
    for copy in copies:
        copy.wait()


def place_part(table, place, parts, start, slots, width, whole):
    pieces, rows, columns = parts[0].shape
    extra = [] if whole is None else [whole]
    return pl.pallas_call(
        functools.partial(place_kernel, start, slots, width),
        out_shape=jax.ShapeDtypeStruct((rows, 4 * slots * columns), jnp.bfloat16),
        in_specs=[SMEM, SMEM] + [VMEM] * 4 + [HBM] * len(extra),
        out_specs=HBM,
        scratch_shapes=[pltpu.SemaphoreType.DMA((4, pieces))],
        input_output_aliases={6: 0} if extra else {},
        compiler_params=GRANT,
        cost_estimate=estimate(1),
    )(table, place, *parts, *extra)


def fast(
    seq_size, hidden, norm_gain, w_query, w_key, w_value, bias_query, bias_key,
    bias_value, w_out,
):
    rows, width = hidden.shape
    depth = w_query.shape[0]
    slots = seq_size // 2
    shard = lax.axis_index("seq")
    side = lax.axis_index("head")
    table = jnp.stack(slot_shards(seq_size, shard) + slot_shards(seq_size, shard, -1))
    place = jnp.reshape(side, (1,)).astype(jnp.int32)

    w_kv = jnp.concatenate([w_key, w_value], axis=1)
    w_kv_other = swap_core(w_kv, seq_size)
    kv_weights = ring_gather(w_kv, w_kv_other, seq_size)
    mine, for_other = norm(table, hidden, norm_gain.reshape(1, width), slots, depth)
    positions = shard * rows + jnp.arange(rows, dtype=jnp.int32)
    half_dim = HEAD_DIM // 2
    freq = ROPE_BASE ** (-2.0 * jnp.arange(half_dim, dtype=jnp.float32) / HEAD_DIM)
    angles = positions.astype(jnp.float32)[:, None] * freq[None, :]
    cosine = jnp.cos(angles)
    sine = jnp.sin(angles)
    cosine = jnp.concatenate([cosine, cosine], axis=1)
    sine = jnp.concatenate([-sine, sine], axis=1)

    bias_kv = jnp.concatenate([bias_key, bias_value]).astype(jnp.float32)[None]
    bias_query = bias_query.astype(jnp.float32)[None]
    for_other, cosine, sine, bias_kv, bias_query = lax.optimization_barrier(
        (for_other, cosine, sine, bias_kv, bias_query)
    )
    other = swap_core(for_other, seq_size)

    keep, send = project(mine, other, kv_weights, 0, ())
    got = swap_core(send, seq_size)
    own_kv = keys_values(keep, got, bias_kv, cosine, sine)
    other_kv = swap_core(own_kv, seq_size)
    held = ring_gather(own_kv, other_kv, seq_size, -1)
    swapped = [other_kv]
    for one in held[1:]:
        swapped.append(swap_core(one, seq_size))

    w_query_other = swap_core(w_query, seq_size)
    q_weights = ring_gather(w_query, w_query_other, seq_size)
    early = slots - 3
    sums = project(mine, other, q_weights[:early], 0, ())
    keep, send = project(mine, other, q_weights[early:], early, sums)
    got = swap_core(send, seq_size)
    query = queries(keep, got, bias_query, cosine, sine)
    state = attend(table, query, held, 2 * slots, ())
    attended = attend(table, query, swapped, 3 * slots, state)

    columns = w_out.shape[1] // 2
    near = lax.dynamic_slice_in_dim(w_out, side * columns, columns, 1)
    far = lax.dynamic_slice_in_dim(w_out, (1 - side) * columns, columns, 1)
    far = swap_head(far)
    piece = jnp.concatenate([near, far])
    piece_other = swap_core(piece, seq_size)
    out_weights = ring_gather(piece, piece_other, seq_size)

    across = swap_head(attended)
    attended_other = swap_core(attended, seq_size)
    across_other = swap_core(across, seq_size)
    operands = (attended, across, attended_other, across_other)
    whole = None
    start = 0
    for count in (slots - 3, 3):
        keep, keep_other, send, send_other = project_out(
            place, operands, out_weights[start : start + count]
        )
        got = swap_head(send)
        got_other = swap_both(send_other, seq_size)
        kept_other = swap_core(keep_other, seq_size)
        whole = place_part(
            table, place, (keep, got, kept_other, got_other), start, slots,
            w_out.shape[1], whole,
        )
        start += count
    return whole


def rotary(values, positions):
    half_dim = values.shape[-1] // 2
    freq = ROPE_BASE ** (-2.0 * jnp.arange(half_dim, dtype=jnp.float32) / values.shape[-1])
    angles = positions.astype(jnp.float32)[:, None, None] * freq[None, None, :]
    cosine = jnp.cos(angles)
    sine = jnp.sin(angles)
    first = values[..., :half_dim]
    second = values[..., half_dim:]
    return jnp.concatenate(
        [first * cosine - second * sine, second * cosine + first * sine], axis=-1
    )


def plain(hidden, norm_gain, w_query, w_key, w_value, bias_query, bias_key, bias_value, w_out):
    rows = hidden.shape[0]
    heads = w_query.shape[1] // HEAD_DIM
    positions = lax.axis_index("seq") * rows + jnp.arange(rows, dtype=jnp.int32)
    widened = hidden.astype(jnp.float32)
    inverse = lax.rsqrt(jnp.mean(widened * widened, axis=-1, keepdims=True) + EPSILON)
    normed = (widened * inverse * norm_gain.astype(jnp.float32)).astype(jnp.bfloat16)
    weights = jnp.concatenate([w_query, w_key, w_value], axis=1)
    biases = jnp.concatenate([bias_query, bias_key, bias_value]).astype(jnp.float32)
    weights = lax.all_gather(weights, "seq", axis=0, tiled=True)
    qkv = jnp.dot(normed, weights, preferred_element_type=jnp.float32) + biases
    query, keys, values = jnp.split(
        qkv, [heads * HEAD_DIM, (heads + 1) * HEAD_DIM], axis=1
    )
    query = rotary(query.reshape(rows, heads, HEAD_DIM), positions).astype(jnp.bfloat16)
    keys = rotary(keys.reshape(rows, 1, HEAD_DIM), positions).reshape(rows, HEAD_DIM)
    pair = jnp.concatenate([keys, values], axis=1).astype(jnp.bfloat16)
    pair = lax.all_gather(pair, "seq", axis=0, tiled=True)
    scores = jnp.einsum(
        "qhd,kd->hqk", query, pair[:, :HEAD_DIM], preferred_element_type=jnp.float32
    )
    allowed = positions[:, None] >= jnp.arange(pair.shape[0], dtype=jnp.int32)[None, :]
    scores = jnp.where(allowed[None], scores * HEAD_DIM ** (-0.5), -jnp.inf)
    probs = jnp.exp(scores - jnp.max(scores, axis=-1, keepdims=True))
    total = jnp.sum(probs, axis=-1, keepdims=True)
    mixed = jnp.einsum(
        "hqk,kd->hqd",
        probs.astype(jnp.bfloat16),
        pair[:, HEAD_DIM:],
        preferred_element_type=jnp.float32,
    )
    attended = (mixed / total).astype(jnp.bfloat16)
    attended = attended.transpose(1, 0, 2).reshape(rows, heads * HEAD_DIM)
    partial_out = jnp.dot(
        attended,
        lax.all_gather(w_out, "seq", axis=1, tiled=True),
        preferred_element_type=jnp.float32,
    )
    return lax.psum_scatter(
        partial_out.astype(jnp.bfloat16), "head", scatter_dimension=0, tiled=True
    )


def local(seq_size, head_size, *args):
    hidden, w_query, w_out = args[0], args[2], args[8]
    fits = (
        head_size == 2
        and seq_size % 4 == 0
        and seq_size >= 8
        and hidden.shape[0] % 32 == 0
        and w_query.shape[0] % 128 == 0
        and w_out.shape[1] % 256 == 0
    )
    if fits:
        return fast(seq_size, *args)
    return plain(*args)


def solution(mesh):
    in_specs = (
        P("seq", None),
        P(),
        P("seq", "head"),
        P("seq", "head"),
        P("seq", "head"),
        P("head"),
        P("head"),
        P("head"),
        P("head", "seq"),
    )
    out_specs = P(("seq", "head"), None)
    body = functools.partial(local, mesh.shape["seq"], mesh.shape["head"])
    return jax.shard_map(
        body, mesh=mesh, in_specs=in_specs, out_specs=out_specs, check_vma=False
    )
```

```python
import functools

import jax
import jax.numpy as jnp
from jax import lax
from jax.experimental import pallas as pl
from jax.experimental.pallas import tpu as pltpu
from jax.sharding import PartitionSpec as P

HEAD_DIM = 128
ROPE_BASE = 1000000.0
EPSILON = 1e-06
LOG2E = 1.4426950408889634


VMEM = pl.BlockSpec(memory_space=pltpu.VMEM)
SMEM = pl.BlockSpec(memory_space=pltpu.SMEM)
HBM = pl.BlockSpec(memory_space=pltpu.HBM)


GRANT = pltpu.CompilerParams(vmem_limit_bytes=28 << 20)


def estimate(microseconds):
    return pl.CostEstimate(
        flops=microseconds * 10**9, bytes_accessed=10**6, transcendentals=0
    )


def dot(a, b, dims=((1,), (0,))):
    return lax.dot_general(a, b, (dims, ((), ())), preferred_element_type=jnp.float32)


def ring_place(seq_size, shard):
    rows = seq_size // 4
    chip = shard // 2
    return jnp.where(chip % 2 == 0, chip // 2, 2 * rows - 1 - chip // 2)


def ring_chip(seq_size, place):
    rows = seq_size // 4
    if place < rows:
        return 2 * place
    return 2 * (2 * rows - 1 - place) + 1


def ring_perm(seq_size, turn):
    chips = seq_size // 2
    pairs = []
    for place in range(chips):
        here = ring_chip(seq_size, place) * 2
        pairs.append((here, ring_chip(seq_size, (place + turn) % chips) * 2))
        pairs.append((here + 1, ring_chip(seq_size, (place - turn) % chips) * 2 + 1))
    return pairs


def slot_shards(seq_size, shard, turn=1):
    chips = seq_size // 2
    rows = seq_size // 4
    place = ring_place(seq_size, shard)
    core = shard % 2
    out = []
    for which in (core, 1 - core):
        way = jnp.where(which == 0, -turn, turn)
        for step in range(chips // 2 + 1):
            at = (place + way * step) % chips
            chip = jnp.where(at < rows, 2 * at, 2 * (2 * rows - 1 - at) + 1)
            out.append(chip * 2 + which)
            if 0 < step < chips // 2:
                out.append(chip * 2 + 1 - which)
    return out


def swap_core(value, seq_size):
    return lax.ppermute(value, "seq", [(s, s ^ 1) for s in range(seq_size)])


def swap_head(value):
    return lax.ppermute(value, "head", [(0, 1), (1, 0)])


def swap_both(value, seq_size):
    pairs = [(i, (((i // 2) ^ 1) * 2) + (1 - i % 2)) for i in range(2 * seq_size)]
    return lax.ppermute(value, ("seq", "head"), pairs)


def pass_on(value, seq_size, turn):
    return lax.ppermute(value, "seq", ring_perm(seq_size, turn))


def ring_gather(own, other, seq_size, turn=1):
    half = seq_size // 4
    held = [own]
    first, second = own, other
    for step in range(1, half + 1):
        first = pass_on(first, seq_size, turn)
        held.append(first)
        if step < half:
            second = pass_on(second, seq_size, turn)
            held.append(second)
    return held


def prepare_kernel(place, w_key, w_value, w_query, w_out, pair, *refs):
    parts, (near, far, sems) = refs[:-3], refs[-3:]
    columns = near.shape[1]
    width = parts[0].shape[1]
    here = pl.multiple_of(place[0] * columns, 128)
    there = pl.multiple_of((1 - place[0]) * columns, 128)
    copies = [
        (w_key, pair.at[:, :HEAD_DIM]),
        (w_value, pair.at[:, HEAD_DIM:]),
        (w_out.at[:, pl.ds(here, columns)], near),
        (w_out.at[:, pl.ds(there, columns)], far),
    ]
    for index, part in enumerate(parts):
        span = slice(index * width, (index + 1) * width)
        copies.append((w_query.at[:, span], part))
    copies = [
        pltpu.make_async_copy(old, new, sems.at[index])
        for index, (old, new) in enumerate(copies)
    ]
    for copy in copies:
        copy.start()
    for copy in copies:
        copy.wait()


def prepare(place, w_key, w_value, w_query, w_out, groups):
    depth, width = w_query.shape
    shapes = [(depth, 2 * HEAD_DIM)] + [(depth, width // groups)] * groups
    shapes += [(w_out.shape[0], w_out.shape[1] // 2)] * 2
    return pl.pallas_call(
        prepare_kernel,
        out_shape=[jax.ShapeDtypeStruct(one, jnp.bfloat16) for one in shapes],
        in_specs=[SMEM] + [HBM] * 4,
        out_specs=[VMEM] * len(shapes),
        scratch_shapes=[pltpu.SemaphoreType.DMA((4 + groups,))],
        cost_estimate=estimate(1),
        name="prep",
    )(place, w_key, w_value, w_query, w_out)


def norm_kernel(table, hidden, gain, mine, other):
    slots, rows, depth = mine.shape
    width = hidden.shape[1]

    def columns_of(index):
        return pl.ds(pl.multiple_of(index * depth, depth), depth)

    def square(index, squares):
        part = hidden[:, columns_of(index)].astype(jnp.float32)
        part = part * part
        for lane in range(0, depth, 128):
            squares = squares + part[:, lane : lane + 128]
        return squares

    squares = jnp.zeros((rows, 128), jnp.float32)
    squares = lax.fori_loop(0, width // depth, square, squares)
    mean = jnp.sum(squares, axis=1, keepdims=True) * (1.0 / width)
    inverse = lax.rsqrt(mean + EPSILON)
    for start, target in ((0, mine), (slots, other)):

        @pl.loop(0, slots)
        def _(slot, start=start, target=target):
            columns = columns_of(table[start + slot])
            value = hidden[:, columns].astype(jnp.float32) * inverse
            value = value * gain[:, columns].astype(jnp.float32)
            target[slot] = value.astype(jnp.bfloat16)


def norm(table, hidden, gain, slots, depth):
    rows = hidden.shape[0]
    shape = jax.ShapeDtypeStruct((slots, rows, depth), jnp.bfloat16)
    return pl.pallas_call(
        norm_kernel,
        out_shape=(shape, shape),
        in_specs=[SMEM, VMEM, VMEM],
        out_specs=(VMEM, VMEM),
        compiler_params=GRANT,
        cost_estimate=estimate(4),
        name="norm",
    )(table, hidden, gain)


def project_kernel(start, count, mine, other, *refs):
    weights = refs[:count]
    keep, send = refs[-2:]
    carried = refs[count:-2]
    for source, target, old in zip(
        (other, mine), (send, keep), carried[::-1] or (None, None)
    ):
        total = None if old is None else old[...]
        for slot in range(count):
            term = dot(source[start + slot], weights[slot][...])
            total = term if total is None else total + term
        target[...] = total


def project(mine, other, weights, start, carried):
    count = len(weights)
    shape = (mine.shape[1], weights[0].shape[1])
    shape = jax.ShapeDtypeStruct(shape, jnp.float32)
    return pl.pallas_call(
        functools.partial(project_kernel, start, count),
        out_shape=(shape, shape),
        in_specs=[VMEM] * (2 + count + len(carried)),
        out_specs=(VMEM, VMEM),
        compiler_params=GRANT,
        cost_estimate=estimate(4),
    )(mine, other, *weights, *carried)


def rotated(value, cosine, sine):
    return value * cosine + pltpu.roll(value, HEAD_DIM // 2, 1) * sine


def keys_values_kernel(keep, got, bias, cosine, sine, out):
    total = keep[...] + got[...] + bias[...]
    out[:, :HEAD_DIM] = rotated(total[:, :HEAD_DIM], cosine[...], sine[...]).astype(
        jnp.bfloat16
    )
    out[:, HEAD_DIM:] = total[:, HEAD_DIM:].astype(jnp.bfloat16)


def keys_values(keep, got, bias, cosine, sine):
    return pl.pallas_call(
        keys_values_kernel,
        out_shape=jax.ShapeDtypeStruct(keep.shape, jnp.bfloat16),
        in_specs=[VMEM] * 5,
        out_specs=VMEM,
        compiler_params=GRANT,
        cost_estimate=estimate(1),
        name="kv",
    )(keep, got, bias, cosine, sine)


def query_kernel(keep, got, bias, cosine, sine, out):
    parts = []
    for column in range(0, keep.shape[1], HEAD_DIM):
        span = slice(column, column + HEAD_DIM)
        value = keep[:, span] + got[:, span] + bias[:, span]
        parts.append(rotated(value, cosine[...], sine[...]))
    out[...] = jnp.concatenate(parts, axis=0).T.astype(jnp.bfloat16)


def queries(keep, got, bias, cosine, sine):
    rows, columns = keep.shape
    shape = (HEAD_DIM, rows * columns // HEAD_DIM)
    return pl.pallas_call(
        query_kernel,
        out_shape=jax.ShapeDtypeStruct(shape, jnp.bfloat16),
        in_specs=[VMEM] * 5,
        out_specs=VMEM,
        compiler_params=GRANT,
        cost_estimate=estimate(2),
    )(keep, got, bias, cosine, sine)


def attend_kernel(count, offset, table, query, *refs):
    sources = refs[:count]
    out, pairs, sems, even, odd, high, weight, mixture = refs[count:]
    rows = sources[0].shape[0]
    lanes = query.shape[1]
    shard = table[0]
    factor = HEAD_DIM ** (-0.5) * LOG2E

    def copy(slot, at):
        pltpu.make_async_copy(sources[slot], pairs.at[at], sems.at[at]).start()

    def wait(at):
        pltpu.make_async_copy(pairs.at[at], pairs.at[at], sems.at[at]).wait()

    copy(0, 0)
    needed = jnp.int32(0)
    for slot in range(1, count):
        seen = table[offset + slot] < shard

        @pl.when(seen)
        def _(slot=slot, needed=needed):
            copy(slot, needed + 1)

        needed = needed + seen.astype(jnp.int32)

    def keys_of(at, size):
        return pairs[pl.ds(at, size), :, :HEAD_DIM].reshape(size * rows, HEAD_DIM)

    def values_of(at, size):
        return pairs[pl.ds(at, size), :, HEAD_DIM:].reshape(size * rows, HEAD_DIM).T

    def update(scores, values, fresh):
        top = jnp.max(scores, axis=0, keepdims=True)
        if not fresh:
            top = jnp.maximum(top, high[...])
        probs = jnp.exp2((scores - top) * factor)
        added = jnp.sum(probs, axis=0, keepdims=True)
        mixed = dot(values, probs.astype(jnp.bfloat16))
        if not fresh:
            scale = jnp.exp2((high[...] - top) * factor)
            added = added + weight[...] * scale
            mixed = mixed + mixture[...] * scale
        high[...] = top
        weight[...] = added
        mixture[...] = mixed

    wait(0)
    scores = dot(keys_of(0, 1), query[...])
    row = lax.broadcasted_iota(jnp.int32, scores.shape, 0)
    lane = lax.rem(lax.broadcasted_iota(jnp.int32, (1, lanes), 1), rows)
    update(jnp.where(row <= lane, scores, -jnp.inf), values_of(0, 1), True)

    single = lax.rem(needed, 2)

    @pl.when(single == 1)
    def _():
        wait(1)
        update(dot(keys_of(1, 1), query[...]), values_of(1, 1), False)

    begin = 1 + single
    turns = needed // 2

    def arrive(turn):
        wait(begin + 2 * turn)
        wait(begin + 2 * turn + 1)

    def step(turn, here, there):
        @pl.when(turn + 1 < turns)
        def _():
            arrive(turn + 1)

        at = begin + 2 * jnp.minimum(turn + 1, turns - 1)
        there[...] = dot(keys_of(at, 2), query[...])
        update(here[...], values_of(begin + 2 * turn, 2), False)

    @pl.when(turns > 0)
    def _():
        arrive(0)
        even[...] = dot(keys_of(begin, 2), query[...])

        @pl.loop(0, (turns + 1) // 2)
        def _(index):
            step(2 * index, even, odd)

            @pl.when(2 * index + 1 < turns)
            def _():
                step(2 * index + 1, odd, even)

    value = (mixture[...] / weight[...]).T
    for head in range(lanes // rows):
        out[:, head * HEAD_DIM : (head + 1) * HEAD_DIM] = value[
            head * rows : (head + 1) * rows
        ].astype(jnp.bfloat16)


def attend(table, query, sources, offset):
    count = len(sources)
    lanes = query.shape[1]
    rows = sources[0].shape[0]
    shape = (rows, lanes // rows * HEAD_DIM)
    return pl.pallas_call(
        functools.partial(attend_kernel, count, offset),
        out_shape=jax.ShapeDtypeStruct(shape, jnp.bfloat16),
        in_specs=[SMEM, VMEM] + [HBM] * count,
        out_specs=VMEM,
        scratch_shapes=[
            pltpu.VMEM((count, rows, 2 * HEAD_DIM), jnp.bfloat16),
            pltpu.SemaphoreType.DMA((count,)),
            pltpu.VMEM((2 * rows, lanes), jnp.float32),
            pltpu.VMEM((2 * rows, lanes), jnp.float32),
            pltpu.VMEM((1, lanes), jnp.float32),
            pltpu.VMEM((1, lanes), jnp.float32),
            pltpu.VMEM((HEAD_DIM, lanes), jnp.float32),
        ],
        compiler_params=GRANT,
        cost_estimate=estimate(8),
    )(table, query, *sources)


def out_kernel(pieces, groups, place, *refs):
    weights = refs[4 * groups : 4 * groups + pieces]
    keep, keep_other, send, send_other, source, block, sems, weight_sems = refs[-8:]
    rows = refs[0].shape[0] // 2
    width = refs[0].shape[1]
    depth = width * groups
    half = place[0]
    near = pl.ds(pl.multiple_of(half * rows, 16), rows)
    far = pl.ds(pl.multiple_of((1 - half) * rows, 16), rows)
    copies = []
    for side in range(2):
        for index in range(groups):
            own, other = refs[side * groups + index], refs[(2 + side) * groups + index]
            for part, (ref, span) in enumerate(
                ((own, near), (other, near), (own, far), (other, far))
            ):
                place_at = (side, pl.ds(part * rows, rows), pl.ds(index * width, width))
                copies.append(
                    pltpu.make_async_copy(
                        ref.at[span], source.at[place_at], sems.at[side, index, part]
                    )
                )
    for copy in copies:
        copy.start()
    for piece in range(pieces):
        pltpu.make_async_copy(
            weights[piece], block.at[piece], weight_sems.at[piece]
        ).start()
    for copy in copies:
        copy.wait()

    @pl.loop(0, pieces)
    def _(piece):
        pltpu.make_async_copy(
            block.at[piece], block.at[piece], weight_sems.at[piece]
        ).wait()
        one = dot(source[0], block[piece, :depth]).astype(jnp.bfloat16)
        two = dot(source[1], block[piece, depth:]).astype(jnp.bfloat16)
        value = (one.astype(jnp.float32) + two.astype(jnp.float32)).astype(jnp.bfloat16)
        for part, target in enumerate((keep, keep_other, send, send_other)):
            target[piece] = value[part * rows : (part + 1) * rows]


def project_out(place, attended, weights):
    pieces = len(weights)
    groups = len(attended) // 4
    rows, depth = attended[0].shape[0], weights[0].shape[0] // 2
    columns = weights[0].shape[1]
    shape = jax.ShapeDtypeStruct((pieces, rows // 2, columns), jnp.bfloat16)
    return pl.pallas_call(
        functools.partial(out_kernel, pieces, groups),
        out_shape=(shape,) * 4,
        in_specs=[SMEM] + [HBM] * (4 * groups + pieces),
        out_specs=(VMEM,) * 4,
        scratch_shapes=[
            pltpu.VMEM((2, 2 * rows, depth), jnp.bfloat16),
            pltpu.VMEM((pieces, 2 * depth, columns), jnp.bfloat16),
            pltpu.SemaphoreType.DMA((2, groups, 4)),
            pltpu.SemaphoreType.DMA((pieces,)),
        ],
        compiler_params=GRANT,
        cost_estimate=estimate(3),
    )(place, *attended, *weights)


def place_kernel(start, slots, width, table, place, *refs):
    keep, got, other, across = refs[:4]
    out, sems = refs[-2:]
    pieces, _, columns = keep.shape
    half = place[0]
    copies = []
    for piece in range(pieces):
        here = table[start + piece] * width
        there = table[slots + start + piece] * width
        for index, (value, base, side) in enumerate(
            (
                (keep, here, half),
                (got, here, 1 - half),
                (other, there, half),
                (across, there, 1 - half),
            )
        ):
            at = pl.multiple_of(base + side * columns, columns)
            copies.append(
                pltpu.make_async_copy(
                    value.at[piece], out.at[:, pl.ds(at, columns)], sems.at[index, piece]
                )
            )
    for copy in copies:
        copy.start()
    for copy in copies:
        copy.wait()


def place_part(table, place, parts, start, slots, width, whole):
    pieces, rows, columns = parts[0].shape
    extra = [] if whole is None else [whole]
    return pl.pallas_call(
        functools.partial(place_kernel, start, slots, width),
        out_shape=jax.ShapeDtypeStruct((rows, 4 * slots * columns), jnp.bfloat16),
        in_specs=[SMEM, SMEM] + [VMEM] * 4 + [HBM] * len(extra),
        out_specs=HBM,
        scratch_shapes=[pltpu.SemaphoreType.DMA((4, pieces))],
        input_output_aliases={6: 0} if extra else {},
        compiler_params=GRANT,
        cost_estimate=estimate(1),
    )(table, place, *parts, *extra)


def fast(
    seq_size, hidden, norm_gain, w_query, w_key, w_value, bias_query, bias_key,
    bias_value, w_out,
):
    rows, width = hidden.shape
    depth = w_query.shape[0]
    slots = seq_size // 2
    groups = 2
    shard = lax.axis_index("seq")
    side = lax.axis_index("head")
    table = jnp.stack(slot_shards(seq_size, shard) + slot_shards(seq_size, shard, -1))
    place = jnp.reshape(side, (1,)).astype(jnp.int32)

    w_kv, *w_queries, near, far = prepare(place, w_key, w_value, w_query, w_out, groups)
    w_kv_other = swap_core(w_kv, seq_size)
    kv_weights = ring_gather(w_kv, w_kv_other, seq_size)
    q_weights = []
    for weight in w_queries:
        weight_other = swap_core(weight, seq_size)
        q_weights.append(ring_gather(weight, weight_other, seq_size))
    mine, for_other = norm(table, hidden, norm_gain.reshape(1, width), slots, depth)

    positions = shard * rows + jnp.arange(rows, dtype=jnp.int32)
    half_dim = HEAD_DIM // 2
    freq = ROPE_BASE ** (-2.0 * jnp.arange(half_dim, dtype=jnp.float32) / HEAD_DIM)
    angles = positions.astype(jnp.float32)[:, None] * freq[None, :]
    cosine = jnp.cos(angles)
    sine = jnp.sin(angles)
    cosine = jnp.concatenate([cosine, cosine], axis=1)
    sine = jnp.concatenate([-sine, sine], axis=1)
    bias_kv = jnp.concatenate([bias_key, bias_value]).astype(jnp.float32)[None]
    bias_query = bias_query.astype(jnp.float32)[None]
    for_other, cosine, sine, bias_kv, bias_query = lax.optimization_barrier(
        (for_other, cosine, sine, bias_kv, bias_query)
    )
    other = swap_core(for_other, seq_size)

    keep, send = project(mine, other, kv_weights, 0, ())
    got = swap_core(send, seq_size)
    own_kv = keys_values(keep, got, bias_kv, cosine, sine)
    other_kv = swap_core(own_kv, seq_size)
    held = ring_gather(own_kv, other_kv, seq_size, -1)
    tokens = held + [other_kv]
    for one in held[1:]:
        tokens.append(swap_core(one, seq_size))

    columns = w_query.shape[1] // groups
    attended = []
    for index, weights in enumerate(q_weights):
        sums = ()
        start = 0
        for count in (slots - 3, 3):
            sums = project(mine, other, weights[start : start + count], start, sums)
            start += count
        keep, send = sums
        got = swap_core(send, seq_size)
        bias = bias_query[:, index * columns : (index + 1) * columns]
        query = queries(keep, got, bias, cosine, sine)
        attended.append(attend(table, query, tokens, 2 * slots))

    far = swap_head(far)
    piece = jnp.concatenate([near, far])
    piece_other = swap_core(piece, seq_size)
    out_weights = ring_gather(piece, piece_other, seq_size)

    across, attended_other, across_other = [], [], []
    for one in attended:
        across.append(swap_head(one))
        attended_other.append(swap_core(one, seq_size))
        across_other.append(swap_core(across[-1], seq_size))
    operands = attended + across + attended_other + across_other
    whole = None
    start = 0
    for count in (slots - 5, 2, 2, 1):
        keep, keep_other, send, send_other = project_out(
            place, operands, out_weights[start : start + count]
        )
        got = swap_head(send)
        got_other = swap_both(send_other, seq_size)
        kept_other = swap_core(keep_other, seq_size)
        whole = place_part(
            table, place, (keep, got, kept_other, got_other), start, slots,
            w_out.shape[1], whole,
        )
        start += count
    return whole


def rotary(values, positions):
    half_dim = values.shape[-1] // 2
    freq = ROPE_BASE ** (-2.0 * jnp.arange(half_dim, dtype=jnp.float32) / values.shape[-1])
    angles = positions.astype(jnp.float32)[:, None, None] * freq[None, None, :]
    cosine = jnp.cos(angles)
    sine = jnp.sin(angles)
    first = values[..., :half_dim]
    second = values[..., half_dim:]
    return jnp.concatenate(
        [first * cosine - second * sine, second * cosine + first * sine], axis=-1
    )


def plain(hidden, norm_gain, w_query, w_key, w_value, bias_query, bias_key, bias_value, w_out):
    rows = hidden.shape[0]
    heads = w_query.shape[1] // HEAD_DIM
    positions = lax.axis_index("seq") * rows + jnp.arange(rows, dtype=jnp.int32)
    widened = hidden.astype(jnp.float32)
    inverse = lax.rsqrt(jnp.mean(widened * widened, axis=-1, keepdims=True) + EPSILON)
    normed = (widened * inverse * norm_gain.astype(jnp.float32)).astype(jnp.bfloat16)
    weights = jnp.concatenate([w_query, w_key, w_value], axis=1)
    biases = jnp.concatenate([bias_query, bias_key, bias_value]).astype(jnp.float32)
    weights = lax.all_gather(weights, "seq", axis=0, tiled=True)
    qkv = jnp.dot(normed, weights, preferred_element_type=jnp.float32) + biases
    query, keys, values = jnp.split(
        qkv, [heads * HEAD_DIM, (heads + 1) * HEAD_DIM], axis=1
    )
    query = rotary(query.reshape(rows, heads, HEAD_DIM), positions).astype(jnp.bfloat16)
    keys = rotary(keys.reshape(rows, 1, HEAD_DIM), positions).reshape(rows, HEAD_DIM)
    pair = jnp.concatenate([keys, values], axis=1).astype(jnp.bfloat16)
    pair = lax.all_gather(pair, "seq", axis=0, tiled=True)
    scores = jnp.einsum(
        "qhd,kd->hqk", query, pair[:, :HEAD_DIM], preferred_element_type=jnp.float32
    )
    allowed = positions[:, None] >= jnp.arange(pair.shape[0], dtype=jnp.int32)[None, :]
    scores = jnp.where(allowed[None], scores * HEAD_DIM ** (-0.5), -jnp.inf)
    probs = jnp.exp(scores - jnp.max(scores, axis=-1, keepdims=True))
    total = jnp.sum(probs, axis=-1, keepdims=True)
    mixed = jnp.einsum(
        "hqk,kd->hqd",
        probs.astype(jnp.bfloat16),
        pair[:, HEAD_DIM:],
        preferred_element_type=jnp.float32,
    )
    attended = (mixed / total).astype(jnp.bfloat16)
    attended = attended.transpose(1, 0, 2).reshape(rows, heads * HEAD_DIM)
    partial_out = jnp.dot(
        attended,
        lax.all_gather(w_out, "seq", axis=1, tiled=True),
        preferred_element_type=jnp.float32,
    )
    return lax.psum_scatter(
        partial_out.astype(jnp.bfloat16), "head", scatter_dimension=0, tiled=True
    )


def local(seq_size, head_size, *args):
    hidden, w_query, w_out = args[0], args[2], args[8]
    fits = (
        head_size == 2
        and seq_size % 4 == 0
        and seq_size >= 8
        and hidden.shape[0] % 32 == 0
        and w_query.shape[0] % 128 == 0
        and w_out.shape[1] % 256 == 0
    )
    if fits:
        return fast(seq_size, *args)
    return plain(*args)


def solution(mesh):
    in_specs = (
        P("seq", None),
        P(),
        P("seq", "head"),
        P("seq", "head"),
        P("seq", "head"),
        P("head"),
        P("head"),
        P("head"),
        P("head", "seq"),
    )
    out_specs = P(("seq", "head"), None)
    body = functools.partial(local, mesh.shape["seq"], mesh.shape["head"])
    return jax.shard_map(
        body, mesh=mesh, in_specs=in_specs, out_specs=out_specs, check_vma=False
    )
```

```python
import functools

import jax
import jax.numpy as jnp
from jax import lax
from jax.experimental import pallas as pl
from jax.experimental.pallas import tpu as pltpu
from jax.sharding import PartitionSpec as P

HEAD_DIM = 128
ROPE_BASE = 1000000.0
EPSILON = 1e-06
LOG2E = 1.4426950408889634


VMEM = pl.BlockSpec(memory_space=pltpu.VMEM)
SMEM = pl.BlockSpec(memory_space=pltpu.SMEM)
HBM = pl.BlockSpec(memory_space=pltpu.HBM)


GRANT = pltpu.CompilerParams(vmem_limit_bytes=28 << 20)


def estimate(microseconds):
    return pl.CostEstimate(
        flops=microseconds * 10**9, bytes_accessed=10**6, transcendentals=0
    )


def dot(a, b, dims=((1,), (0,))):
    return lax.dot_general(a, b, (dims, ((), ())), preferred_element_type=jnp.float32)


def ring_place(seq_size, shard):
    rows = seq_size // 4
    chip = shard // 2
    return jnp.where(chip % 2 == 0, chip // 2, 2 * rows - 1 - chip // 2)


def ring_chip(seq_size, place):
    rows = seq_size // 4
    if place < rows:
        return 2 * place
    return 2 * (2 * rows - 1 - place) + 1


def ring_perm(seq_size, turn):
    chips = seq_size // 2
    pairs = []
    for place in range(chips):
        here = ring_chip(seq_size, place) * 2
        pairs.append((here, ring_chip(seq_size, (place + turn) % chips) * 2))
        pairs.append((here + 1, ring_chip(seq_size, (place - turn) % chips) * 2 + 1))
    return pairs


def slot_shards(seq_size, shard, turn=1):
    chips = seq_size // 2
    rows = seq_size // 4
    place = ring_place(seq_size, shard)
    core = shard % 2
    out = []
    for which in (core, 1 - core):
        way = jnp.where(which == 0, -turn, turn)
        for step in range(chips // 2 + 1):
            at = (place + way * step) % chips
            chip = jnp.where(at < rows, 2 * at, 2 * (2 * rows - 1 - at) + 1)
            out.append(chip * 2 + which)
            if 0 < step < chips // 2:
                out.append(chip * 2 + 1 - which)
    return out


def swap_core(value, seq_size):
    return lax.ppermute(value, "seq", [(s, s ^ 1) for s in range(seq_size)])


def swap_head(value):
    return lax.ppermute(value, "head", [(0, 1), (1, 0)])


def swap_both(value, seq_size):
    pairs = [(i, (((i // 2) ^ 1) * 2) + (1 - i % 2)) for i in range(2 * seq_size)]
    return lax.ppermute(value, ("seq", "head"), pairs)


def pass_on(value, seq_size, turn):
    return lax.ppermute(value, "seq", ring_perm(seq_size, turn))


def ring_gather(own, other, seq_size, turn=1, begin=1):
    half = seq_size // 4
    held = [own] if begin == 1 else [own, other]
    first, second = own, other
    for step in range(begin, half + 1):
        first = pass_on(first, seq_size, turn)
        held.append(first)
        if step < half:
            second = pass_on(second, seq_size, turn)
            held.append(second)
    return held


def copy_all(pairs, sems):
    copies = [
        pltpu.make_async_copy(old, new, sems.at[index])
        for index, (old, new) in enumerate(pairs)
    ]
    for copy in copies:
        copy.start()
    for copy in copies:
        copy.wait()


def join_kernel(w_key, w_value, pair, sems):
    copy_all(
        [(w_key, pair.at[:, :HEAD_DIM]), (w_value, pair.at[:, HEAD_DIM:])], sems
    )


def join(w_key, w_value):
    shape = (w_key.shape[0], 2 * HEAD_DIM)
    return pl.pallas_call(
        join_kernel,
        out_shape=jax.ShapeDtypeStruct(shape, jnp.bfloat16),
        in_specs=[HBM] * 2,
        out_specs=VMEM,
        scratch_shapes=[pltpu.SemaphoreType.DMA((2,))],
        cost_estimate=estimate(1),
        name="prep",
    )(w_key, w_value)


def halves_kernel(value, *parts):
    width = parts[0].shape[1]
    for index, part in enumerate(parts):
        part[...] = value[:, index * width : (index + 1) * width]


def halves(value, groups):
    shape = (value.shape[0], value.shape[1] // groups)
    return pl.pallas_call(
        halves_kernel,
        out_shape=[jax.ShapeDtypeStruct(shape, jnp.bfloat16)] * groups,
        in_specs=[VMEM],
        out_specs=[VMEM] * groups,
        compiler_params=GRANT,
        cost_estimate=estimate(1),
    )(value)


def cut_kernel(place, own, got, near, far):
    depth, columns = own.shape[0], near.shape[1]
    for side, target in ((place[0], near), (1 - place[0], far)):
        span = pl.ds(pl.multiple_of(side * columns, 128), columns)
        target[:depth] = own[:, span]
        target[depth:] = got[:, span]


def cut(place, own, got):
    shape = jax.ShapeDtypeStruct((2 * own.shape[0], own.shape[1] // 2), jnp.bfloat16)
    return pl.pallas_call(
        cut_kernel,
        out_shape=(shape, shape),
        in_specs=[SMEM, VMEM, VMEM],
        out_specs=(VMEM, VMEM),
        compiler_params=GRANT,
        cost_estimate=estimate(1),
        name="cut",
    )(place, own, got)


def norm_kernel(table, hidden, gain, mine, other):
    slots, rows, depth = mine.shape
    width = hidden.shape[1]

    def columns_of(index):
        return pl.ds(pl.multiple_of(index * depth, depth), depth)

    def square(index, squares):
        part = hidden[:, columns_of(index)].astype(jnp.float32)
        part = part * part
        for lane in range(0, depth, 128):
            squares = squares + part[:, lane : lane + 128]
        return squares

    squares = jnp.zeros((rows, 128), jnp.float32)
    squares = lax.fori_loop(0, width // depth, square, squares)
    mean = jnp.sum(squares, axis=1, keepdims=True) * (1.0 / width)
    inverse = lax.rsqrt(mean + EPSILON)
    for start, target in ((0, mine), (slots, other)):

        @pl.loop(0, slots)
        def _(slot, start=start, target=target):
            columns = columns_of(table[start + slot])
            value = hidden[:, columns].astype(jnp.float32) * inverse
            value = value * gain[:, columns].astype(jnp.float32)
            target[slot] = value.astype(jnp.bfloat16)


def norm(table, hidden, gain, slots, depth):
    rows = hidden.shape[0]
    shape = jax.ShapeDtypeStruct((slots, rows, depth), jnp.bfloat16)
    return pl.pallas_call(
        norm_kernel,
        out_shape=(shape, shape),
        in_specs=[SMEM, VMEM, VMEM],
        out_specs=(VMEM, VMEM),
        compiler_params=GRANT,
        cost_estimate=estimate(4),
        name="norm",
    )(table, hidden, gain)


def project_kernel(start, count, group, mine, other, *refs):
    weights = refs[:count]
    keep, send = refs[-2:]
    carried = refs[count:-2]
    for source, target, old in zip(
        (other, mine), (send, keep), carried[::-1] or (None, None)
    ):
        total = None if old is None else old[...]
        for slot in range(count):
            columns = target.shape[1]
            at = group * columns if weights[slot].shape[1] > columns else 0
            term = dot(source[start + slot], weights[slot][:, at : at + columns])
            total = term if total is None else total + term
        target[...] = total


def project(mine, other, weights, columns, group, start, carried):
    count = len(weights)
    shape = (mine.shape[1], columns)
    shape = jax.ShapeDtypeStruct(shape, jnp.float32)
    return pl.pallas_call(
        functools.partial(project_kernel, start, count, group),
        out_shape=(shape, shape),
        in_specs=[VMEM] * (2 + count + len(carried)),
        out_specs=(VMEM, VMEM),
        compiler_params=GRANT,
        cost_estimate=estimate(4),
    )(mine, other, *weights, *carried)


def rotated(value, cosine, sine):
    return value * cosine + pltpu.roll(value, HEAD_DIM // 2, 1) * sine


def keys_values_kernel(keep, got, bias, cosine, sine, out):
    total = keep[...] + got[...] + bias[...]
    out[:, :HEAD_DIM] = rotated(total[:, :HEAD_DIM], cosine[...], sine[...]).astype(
        jnp.bfloat16
    )
    out[:, HEAD_DIM:] = total[:, HEAD_DIM:].astype(jnp.bfloat16)


def keys_values(keep, got, bias, cosine, sine):
    return pl.pallas_call(
        keys_values_kernel,
        out_shape=jax.ShapeDtypeStruct(keep.shape, jnp.bfloat16),
        in_specs=[VMEM] * 5,
        out_specs=VMEM,
        compiler_params=GRANT,
        cost_estimate=estimate(1),
        name="kv",
    )(keep, got, bias, cosine, sine)


def query_kernel(keep, got, bias, cosine, sine, out):
    parts = []
    for column in range(0, keep.shape[1], HEAD_DIM):
        span = slice(column, column + HEAD_DIM)
        value = keep[:, span] + got[:, span] + bias[:, span]
        parts.append(rotated(value, cosine[...], sine[...]))
    out[...] = jnp.concatenate(parts, axis=0).T.astype(jnp.bfloat16)


def queries(keep, got, bias, cosine, sine):
    rows, columns = keep.shape
    shape = (HEAD_DIM, rows * columns // HEAD_DIM)
    return pl.pallas_call(
        query_kernel,
        out_shape=jax.ShapeDtypeStruct(shape, jnp.bfloat16),
        in_specs=[VMEM] * 5,
        out_specs=VMEM,
        compiler_params=GRANT,
        cost_estimate=estimate(2),
    )(keep, got, bias, cosine, sine)


def attend_kernel(count, offset, table, query, *refs):
    sources = refs[:count]
    out, pairs, even, odd, high, weight, mixture = refs[count:]
    rows = sources[0].shape[0]
    lanes = query.shape[1]
    shard = table[0]
    factor = HEAD_DIM ** (-0.5) * LOG2E

    needed = jnp.int32(0)
    for slot in range(1, count):
        seen = table[offset + slot] < shard

        @pl.when(seen)
        def _(slot=slot, needed=needed):
            pairs[pl.ds(needed, 1)] = sources[slot][...][None]

        needed = needed + seen.astype(jnp.int32)

    def keys_of(at, size):
        return pairs[pl.ds(at, size), :, :HEAD_DIM].reshape(size * rows, HEAD_DIM)

    def values_of(at, size):
        return pairs[pl.ds(at, size), :, HEAD_DIM:].reshape(size * rows, HEAD_DIM).T

    def update(scores, values, fresh):
        top = jnp.max(scores, axis=0, keepdims=True)
        if not fresh:
            top = jnp.maximum(top, high[...])
        probs = jnp.exp2((scores - top) * factor)
        added = jnp.sum(probs, axis=0, keepdims=True)
        mixed = dot(values, probs.astype(jnp.bfloat16))
        if not fresh:
            scale = jnp.exp2((high[...] - top) * factor)
            added = added + weight[...] * scale
            mixed = mixed + mixture[...] * scale
        high[...] = top
        weight[...] = added
        mixture[...] = mixed

    scores = dot(sources[0][:, :HEAD_DIM], query[...])
    row = lax.broadcasted_iota(jnp.int32, scores.shape, 0)
    lane = lax.rem(lax.broadcasted_iota(jnp.int32, (1, lanes), 1), rows)
    update(jnp.where(row <= lane, scores, -jnp.inf), sources[0][:, HEAD_DIM:].T, True)

    single = lax.rem(needed, 2)

    @pl.when(single == 1)
    def _():
        update(dot(keys_of(0, 1), query[...]), values_of(0, 1), False)

    begin = single
    turns = needed // 2

    def step(turn, here, there):
        at = begin + 2 * jnp.minimum(turn + 1, turns - 1)
        there[...] = dot(keys_of(at, 2), query[...])
        update(here[...], values_of(begin + 2 * turn, 2), False)

    @pl.when(turns > 0)
    def _():
        even[...] = dot(keys_of(begin, 2), query[...])

        @pl.loop(0, (turns + 1) // 2)
        def _(index):
            step(2 * index, even, odd)

            @pl.when(2 * index + 1 < turns)
            def _():
                step(2 * index + 1, odd, even)

    value = (mixture[...] / weight[...]).T
    for head in range(lanes // rows):
        out[:, head * HEAD_DIM : (head + 1) * HEAD_DIM] = value[
            head * rows : (head + 1) * rows
        ].astype(jnp.bfloat16)


def attend(table, query, sources, offset):
    count = len(sources)
    lanes = query.shape[1]
    rows = sources[0].shape[0]
    shape = (rows, lanes // rows * HEAD_DIM)
    return pl.pallas_call(
        functools.partial(attend_kernel, count, offset),
        out_shape=jax.ShapeDtypeStruct(shape, jnp.bfloat16),
        in_specs=[SMEM, VMEM] + [VMEM] * count,
        out_specs=VMEM,
        scratch_shapes=[
            pltpu.VMEM((count, rows, 2 * HEAD_DIM), jnp.bfloat16),
            pltpu.VMEM((2 * rows, lanes), jnp.float32),
            pltpu.VMEM((2 * rows, lanes), jnp.float32),
            pltpu.VMEM((1, lanes), jnp.float32),
            pltpu.VMEM((1, lanes), jnp.float32),
            pltpu.VMEM((HEAD_DIM, lanes), jnp.float32),
        ],
        compiler_params=GRANT,
        cost_estimate=estimate(8),
    )(table, query, *sources)


def out_kernel(pieces, groups, share, place, *refs):
    weights = refs[4 * groups : 4 * groups + pieces]
    targets, source = refs[4 * groups + pieces : -1], refs[-1]
    rows, width = refs[0].shape[0] // 2, refs[0].shape[1]
    depth = width * groups
    near = pl.ds(pl.multiple_of(place[0] * rows, 16), rows)
    far = pl.ds(pl.multiple_of((1 - place[0]) * rows, 16), rows)
    for side in range(2):
        for index in range(groups):
            own, other = refs[side * groups + index], refs[(2 + side) * groups + index]
            columns = slice(index * width, (index + 1) * width)
            for part, (ref, span) in enumerate(
                ((own, near), (other, near), (own, far), (other, far))[: 2 * share]
            ):
                source[side, part * rows : (part + 1) * rows, columns] = ref[span, :]
    for piece in range(pieces):
        block = weights[piece]
        one = dot(source[0], block[:depth]).astype(jnp.bfloat16)
        two = dot(source[1], block[depth:]).astype(jnp.bfloat16)
        value = (one.astype(jnp.float32) + two.astype(jnp.float32)).astype(jnp.bfloat16)
        for part, target in enumerate(targets):
            target[piece] = value[part * rows : (part + 1) * rows]


def project_out(place, attended, weights, share):
    pieces = len(weights)
    groups = len(attended) // 4
    rows, depth = attended[0].shape[0], weights[0].shape[0] // 2
    columns = weights[0].shape[1]
    shape = jax.ShapeDtypeStruct((pieces, rows // 2, columns), jnp.bfloat16)
    return pl.pallas_call(
        functools.partial(out_kernel, pieces, groups, share),
        out_shape=(shape,) * (2 * share),
        in_specs=[SMEM] + [VMEM] * (4 * groups + pieces),
        out_specs=(VMEM,) * (2 * share),
        scratch_shapes=[pltpu.VMEM((2, share * rows, depth), jnp.bfloat16)],
        compiler_params=GRANT,
        cost_estimate=estimate(3),
    )(place, *attended, *weights)


def place_kernel(start, slots, width, table, place, *refs):
    keep, got, other, across = refs[:4]
    out, sems = refs[-2:]
    pieces, _, columns = keep.shape
    half = place[0]
    copies = []
    for piece in range(pieces):
        here = table[start + piece] * width
        there = table[slots + start + piece] * width
        for index, (value, base, side) in enumerate(
            (
                (keep, here, half),
                (got, here, 1 - half),
                (other, there, half),
                (across, there, 1 - half),
            )
        ):
            at = pl.multiple_of(base + side * columns, columns)
            copies.append(
                pltpu.make_async_copy(
                    value.at[piece], out.at[:, pl.ds(at, columns)], sems.at[index, piece]
                )
            )
    for copy in copies:
        copy.start()
    for copy in copies:
        copy.wait()


def place_part(table, place, parts, start, slots, width, whole):
    pieces, rows, columns = parts[0].shape
    extra = [] if whole is None else [whole]
    return pl.pallas_call(
        functools.partial(place_kernel, start, slots, width),
        out_shape=jax.ShapeDtypeStruct((rows, 4 * slots * columns), jnp.bfloat16),
        in_specs=[SMEM, SMEM] + [VMEM] * 4 + [HBM] * len(extra),
        out_specs=HBM,
        scratch_shapes=[pltpu.SemaphoreType.DMA((4, pieces))],
        input_output_aliases={6: 0} if extra else {},
        compiler_params=GRANT,
        cost_estimate=estimate(1),
    )(table, place, *parts, *extra)


def fast(
    seq_size, hidden, norm_gain, w_query, w_key, w_value, bias_query, bias_key,
    bias_value, w_out,
):
    rows, width = hidden.shape
    depth = w_query.shape[0]
    slots = seq_size // 2
    groups = 2
    shard = lax.axis_index("seq")
    side = lax.axis_index("head")
    table = jnp.stack(slot_shards(seq_size, shard) + slot_shards(seq_size, shard, -1))
    place = jnp.reshape(side, (1,)).astype(jnp.int32)

    q_first = pass_on(w_query, seq_size, 1)
    w_query_other = swap_core(w_query, seq_size)
    q_second = pass_on(w_query_other, seq_size, 1)
    q_weights = []
    for first, second in zip(halves(q_first, groups), halves(q_second, groups)):
        ring = ring_gather(first, second, seq_size, begin=2)
        q_weights.append([w_query, q_first, q_second] + ring[2:])
    w_kv = join(w_key, w_value)
    w_kv_other = swap_core(w_kv, seq_size)
    kv_weights = ring_gather(w_kv, w_kv_other, seq_size)
    mine, for_other = norm(table, hidden, norm_gain.reshape(1, width), slots, depth)

    positions = shard * rows + jnp.arange(rows, dtype=jnp.int32)
    half_dim = HEAD_DIM // 2
    freq = ROPE_BASE ** (-2.0 * jnp.arange(half_dim, dtype=jnp.float32) / HEAD_DIM)
    angles = positions.astype(jnp.float32)[:, None] * freq[None, :]
    cosine = jnp.cos(angles)
    sine = jnp.sin(angles)
    cosine = jnp.concatenate([cosine, cosine], axis=1)
    sine = jnp.concatenate([-sine, sine], axis=1)
    bias_kv = jnp.concatenate([bias_key, bias_value]).astype(jnp.float32)[None]
    bias_query = bias_query.astype(jnp.float32)[None]
    for_other, cosine, sine, bias_kv, bias_query = lax.optimization_barrier(
        (for_other, cosine, sine, bias_kv, bias_query)
    )
    other = swap_core(for_other, seq_size)

    keep, send = project(mine, other, kv_weights, 2 * HEAD_DIM, 0, 0, ())
    got = swap_core(send, seq_size)
    own_kv = keys_values(keep, got, bias_kv, cosine, sine)
    other_kv = swap_core(own_kv, seq_size)
    held = ring_gather(own_kv, other_kv, seq_size, -1)
    tokens = held + [other_kv]
    for one in held[1:]:
        tokens.append(swap_core(one, seq_size))

    columns = w_query.shape[1] // groups
    attended = []
    for index, weights in enumerate(q_weights):
        sums = ()
        start = 0
        for count in (slots - 3, 3):
            sums = project(
                mine, other, weights[start : start + count], columns, index, start,
                sums,
            )
            start += count
        keep, send = sums
        got = swap_core(send, seq_size)
        bias = bias_query[:, index * columns : (index + 1) * columns]
        query = queries(keep, got, bias, cosine, sine)
        attended.append(attend(table, query, tokens, 2 * slots))

    w_out_across = swap_head(w_out)
    piece, rest = cut(place, w_out, w_out_across)
    piece_other = swap_core(piece, seq_size)
    out_weights = ring_gather(piece, piece_other, seq_size)

    across, attended_other, across_other = [], [], []
    for one in attended:
        across.append(swap_head(one))
        attended_other.append(swap_core(one, seq_size))
        across_other.append(swap_core(across[-1], seq_size))
    operands = attended + across + attended_other + across_other
    keep, keep_other = project_out(place, operands, (piece, rest), 1)
    theirs = swap_core(keep_other, seq_size)
    parts = (keep[:1], keep[1:], theirs[:1], theirs[1:])
    whole = place_part(table, place, parts, 0, slots, w_out.shape[1], None)
    start = 1
    for count in (slots - 6, 2, 2, 1):
        keep, keep_other, send, send_other = project_out(
            place, operands, out_weights[start : start + count], 2
        )
        got = swap_head(send)
        got_other = swap_both(send_other, seq_size)
        kept_other = swap_core(keep_other, seq_size)
        whole = place_part(
            table, place, (keep, got, kept_other, got_other), start, slots,
            w_out.shape[1], whole,
        )
        start += count
    return whole


def rotary(values, positions):
    half_dim = values.shape[-1] // 2
    freq = ROPE_BASE ** (-2.0 * jnp.arange(half_dim, dtype=jnp.float32) / values.shape[-1])
    angles = positions.astype(jnp.float32)[:, None, None] * freq[None, None, :]
    cosine = jnp.cos(angles)
    sine = jnp.sin(angles)
    first = values[..., :half_dim]
    second = values[..., half_dim:]
    return jnp.concatenate(
        [first * cosine - second * sine, second * cosine + first * sine], axis=-1
    )


def plain(hidden, norm_gain, w_query, w_key, w_value, bias_query, bias_key, bias_value, w_out):
    rows = hidden.shape[0]
    heads = w_query.shape[1] // HEAD_DIM
    positions = lax.axis_index("seq") * rows + jnp.arange(rows, dtype=jnp.int32)
    widened = hidden.astype(jnp.float32)
    inverse = lax.rsqrt(jnp.mean(widened * widened, axis=-1, keepdims=True) + EPSILON)
    normed = (widened * inverse * norm_gain.astype(jnp.float32)).astype(jnp.bfloat16)
    weights = jnp.concatenate([w_query, w_key, w_value], axis=1)
    biases = jnp.concatenate([bias_query, bias_key, bias_value]).astype(jnp.float32)
    weights = lax.all_gather(weights, "seq", axis=0, tiled=True)
    qkv = jnp.dot(normed, weights, preferred_element_type=jnp.float32) + biases
    query, keys, values = jnp.split(
        qkv, [heads * HEAD_DIM, (heads + 1) * HEAD_DIM], axis=1
    )
    query = rotary(query.reshape(rows, heads, HEAD_DIM), positions).astype(jnp.bfloat16)
    keys = rotary(keys.reshape(rows, 1, HEAD_DIM), positions).reshape(rows, HEAD_DIM)
    pair = jnp.concatenate([keys, values], axis=1).astype(jnp.bfloat16)
    pair = lax.all_gather(pair, "seq", axis=0, tiled=True)
    scores = jnp.einsum(
        "qhd,kd->hqk", query, pair[:, :HEAD_DIM], preferred_element_type=jnp.float32
    )
    allowed = positions[:, None] >= jnp.arange(pair.shape[0], dtype=jnp.int32)[None, :]
    scores = jnp.where(allowed[None], scores * HEAD_DIM ** (-0.5), -jnp.inf)
    probs = jnp.exp(scores - jnp.max(scores, axis=-1, keepdims=True))
    total = jnp.sum(probs, axis=-1, keepdims=True)
    mixed = jnp.einsum(
        "hqk,kd->hqd",
        probs.astype(jnp.bfloat16),
        pair[:, HEAD_DIM:],
        preferred_element_type=jnp.float32,
    )
    attended = (mixed / total).astype(jnp.bfloat16)
    attended = attended.transpose(1, 0, 2).reshape(rows, heads * HEAD_DIM)
    partial_out = jnp.dot(
        attended,
        lax.all_gather(w_out, "seq", axis=1, tiled=True),
        preferred_element_type=jnp.float32,
    )
    return lax.psum_scatter(
        partial_out.astype(jnp.bfloat16), "head", scatter_dimension=0, tiled=True
    )


def local(seq_size, head_size, *args):
    hidden, w_query, w_out = args[0], args[2], args[8]
    fits = (
        head_size == 2
        and seq_size % 4 == 0
        and seq_size >= 8
        and hidden.shape[0] % 32 == 0
        and w_query.shape[0] % 128 == 0
        and w_out.shape[1] % 256 == 0
    )
    if fits:
        return fast(seq_size, *args)
    return plain(*args)


def solution(mesh):
    in_specs = (
        P("seq", None),
        P(),
        P("seq", "head"),
        P("seq", "head"),
        P("seq", "head"),
        P("head"),
        P("head"),
        P("head"),
        P("head", "seq"),
    )
    out_specs = P(("seq", "head"), None)
    body = functools.partial(local, mesh.shape["seq"], mesh.shape["head"])
    return jax.shard_map(
        body, mesh=mesh, in_specs=in_specs, out_specs=out_specs, check_vma=False
    )
```

```python
import functools

import jax
import jax.numpy as jnp
from jax import lax
from jax.experimental import pallas as pl
from jax.experimental.pallas import tpu as pltpu
from jax.sharding import PartitionSpec as P

HEAD_DIM = 128
ROPE_BASE = 1000000.0
EPSILON = 1e-06
LOG2E = 1.4426950408889634


VMEM = pl.BlockSpec(memory_space=pltpu.VMEM)
SMEM = pl.BlockSpec(memory_space=pltpu.SMEM)
HBM = pl.BlockSpec(memory_space=pltpu.HBM)


GRANT = pltpu.CompilerParams(vmem_limit_bytes=28 << 20)


def estimate(microseconds):
    return pl.CostEstimate(
        flops=microseconds * 10**9, bytes_accessed=10**6, transcendentals=0
    )


def dot(a, b, dims=((1,), (0,))):
    return lax.dot_general(a, b, (dims, ((), ())), preferred_element_type=jnp.float32)


def ring_place(seq_size, shard):
    rows = seq_size // 4
    chip = shard // 2
    return jnp.where(chip % 2 == 0, chip // 2, 2 * rows - 1 - chip // 2)


def ring_chip(seq_size, place):
    rows = seq_size // 4
    if place < rows:
        return 2 * place
    return 2 * (2 * rows - 1 - place) + 1


def ring_perm(seq_size, turn):
    chips = seq_size // 2
    pairs = []
    for place in range(chips):
        here = ring_chip(seq_size, place) * 2
        pairs.append((here, ring_chip(seq_size, (place + turn) % chips) * 2))
        pairs.append((here + 1, ring_chip(seq_size, (place - turn) % chips) * 2 + 1))
    return pairs


def slot_shards(seq_size, shard, turn=1):
    chips = seq_size // 2
    rows = seq_size // 4
    place = ring_place(seq_size, shard)
    core = shard % 2
    out = []
    for which in (core, 1 - core):
        way = jnp.where(which == 0, -turn, turn)
        for step in range(chips // 2 + 1):
            at = (place + way * step) % chips
            chip = jnp.where(at < rows, 2 * at, 2 * (2 * rows - 1 - at) + 1)
            out.append(chip * 2 + which)
            if 0 < step < chips // 2:
                out.append(chip * 2 + 1 - which)
    return out


def swap_core(value, seq_size):
    return lax.ppermute(value, "seq", [(s, s ^ 1) for s in range(seq_size)])


def swap_head(value):
    return lax.ppermute(value, "head", [(0, 1), (1, 0)])


def swap_both(value, seq_size):
    pairs = [(i, (((i // 2) ^ 1) * 2) + (1 - i % 2)) for i in range(2 * seq_size)]
    return lax.ppermute(value, ("seq", "head"), pairs)


def pass_on(value, seq_size, turn):
    return lax.ppermute(value, "seq", ring_perm(seq_size, turn))


def ring_gather(own, other, seq_size, turn=1, begin=1):
    half = seq_size // 4
    held = [own] if begin == 1 else [own, other]
    first, second = own, other
    for step in range(begin, half + 1):
        first = pass_on(first, seq_size, turn)
        held.append(first)
        if step < half:
            second = pass_on(second, seq_size, turn)
            held.append(second)
    return held


def copy_all(pairs, sems):
    copies = [
        pltpu.make_async_copy(old, new, sems.at[index])
        for index, (old, new) in enumerate(pairs)
    ]
    for copy in copies:
        copy.start()
    for copy in copies:
        copy.wait()


def join_kernel(w_key, w_value, pair, sems):
    copy_all(
        [(w_key, pair.at[:, :HEAD_DIM]), (w_value, pair.at[:, HEAD_DIM:])], sems
    )


def join(w_key, w_value):
    shape = (w_key.shape[0], 2 * HEAD_DIM)
    return pl.pallas_call(
        join_kernel,
        out_shape=jax.ShapeDtypeStruct(shape, jnp.bfloat16),
        in_specs=[HBM] * 2,
        out_specs=VMEM,
        scratch_shapes=[pltpu.SemaphoreType.DMA((2,))],
        cost_estimate=estimate(1),
        name="prep",
    )(w_key, w_value)


def halves_kernel(value, *parts):
    width = parts[0].shape[1]
    for index, part in enumerate(parts):
        part[...] = value[:, index * width : (index + 1) * width]


def halves(value, groups):
    shape = (value.shape[0], value.shape[1] // groups)
    return pl.pallas_call(
        halves_kernel,
        out_shape=[jax.ShapeDtypeStruct(shape, jnp.bfloat16)] * groups,
        in_specs=[VMEM],
        out_specs=[VMEM] * groups,
        compiler_params=GRANT,
        cost_estimate=estimate(1),
    )(value)


def cut_kernel(place, own, got, near, far):
    depth, columns = own.shape[0], near.shape[1]
    for side, target in ((place[0], near), (1 - place[0], far)):
        span = pl.ds(pl.multiple_of(side * columns, 128), columns)
        target[:depth] = own[:, span]
        target[depth:] = got[:, span]


def cut(place, own, got):
    shape = jax.ShapeDtypeStruct((2 * own.shape[0], own.shape[1] // 2), jnp.bfloat16)
    return pl.pallas_call(
        cut_kernel,
        out_shape=(shape, shape),
        in_specs=[SMEM, VMEM, VMEM],
        out_specs=(VMEM, VMEM),
        compiler_params=GRANT,
        cost_estimate=estimate(1),
        name="cut",
    )(place, own, got)


def norm_kernel(table, hidden, gain, mine, other):
    slots, rows, depth = mine.shape
    width = hidden.shape[1]

    def columns_of(index):
        return pl.ds(pl.multiple_of(index * depth, depth), depth)

    def square(index, squares):
        part = hidden[:, columns_of(index)].astype(jnp.float32)
        part = part * part
        for lane in range(0, depth, 128):
            squares = squares + part[:, lane : lane + 128]
        return squares

    squares = jnp.zeros((rows, 128), jnp.float32)
    squares = lax.fori_loop(0, width // depth, square, squares)
    mean = jnp.sum(squares, axis=1, keepdims=True) * (1.0 / width)
    inverse = lax.rsqrt(mean + EPSILON)
    for start, target in ((0, mine), (slots, other)):

        @pl.loop(0, slots)
        def _(slot, start=start, target=target):
            columns = columns_of(table[start + slot])
            value = hidden[:, columns].astype(jnp.float32) * inverse
            value = value * gain[:, columns].astype(jnp.float32)
            target[slot] = value.astype(jnp.bfloat16)


def norm(table, hidden, gain, slots, depth):
    rows = hidden.shape[0]
    shape = jax.ShapeDtypeStruct((slots, rows, depth), jnp.bfloat16)
    return pl.pallas_call(
        norm_kernel,
        out_shape=(shape, shape),
        in_specs=[SMEM, VMEM, VMEM],
        out_specs=(VMEM, VMEM),
        compiler_params=GRANT,
        cost_estimate=estimate(4),
        name="norm",
    )(table, hidden, gain)


def project_kernel(start, count, group, mine, other, *refs):
    weights = refs[:count]
    keep, send = refs[-2:]
    carried = refs[count:-2]
    for source, target, old in zip(
        (other, mine), (send, keep), carried[::-1] or (None, None)
    ):
        total = None if old is None else old[...]
        for slot in range(count):
            columns = target.shape[1]
            at = group * columns if weights[slot].shape[1] > columns else 0
            term = dot(source[start + slot], weights[slot][:, at : at + columns])
            total = term if total is None else total + term
        target[...] = total


def project(mine, other, weights, columns, group, start, carried):
    count = len(weights)
    shape = (mine.shape[1], columns)
    shape = jax.ShapeDtypeStruct(shape, jnp.float32)
    return pl.pallas_call(
        functools.partial(project_kernel, start, count, group),
        out_shape=(shape, shape),
        in_specs=[VMEM] * (2 + count + len(carried)),
        out_specs=(VMEM, VMEM),
        compiler_params=GRANT,
        cost_estimate=estimate(4),
    )(mine, other, *weights, *carried)


def rotated(value, cosine, sine):
    return value * cosine + pltpu.roll(value, HEAD_DIM // 2, 1) * sine


def keys_values_kernel(keep, got, bias, cosine, sine, out):
    total = keep[...] + got[...] + bias[...]
    out[:, :HEAD_DIM] = rotated(total[:, :HEAD_DIM], cosine[...], sine[...]).astype(
        jnp.bfloat16
    )
    out[:, HEAD_DIM:] = total[:, HEAD_DIM:].astype(jnp.bfloat16)


def keys_values(keep, got, bias, cosine, sine):
    return pl.pallas_call(
        keys_values_kernel,
        out_shape=jax.ShapeDtypeStruct(keep.shape, jnp.bfloat16),
        in_specs=[VMEM] * 5,
        out_specs=VMEM,
        compiler_params=GRANT,
        cost_estimate=estimate(1),
        name="kv",
    )(keep, got, bias, cosine, sine)


def query_kernel(keep, got, bias, cosine, sine, out):
    parts = []
    for column in range(0, keep.shape[1], HEAD_DIM):
        span = slice(column, column + HEAD_DIM)
        value = keep[:, span] + got[:, span] + bias[:, span]
        parts.append(rotated(value, cosine[...], sine[...]))
    out[...] = jnp.concatenate(parts, axis=0).T.astype(jnp.bfloat16)


def queries(keep, got, bias, cosine, sine):
    rows, columns = keep.shape
    shape = (HEAD_DIM, rows * columns // HEAD_DIM)
    return pl.pallas_call(
        query_kernel,
        out_shape=jax.ShapeDtypeStruct(shape, jnp.bfloat16),
        in_specs=[VMEM] * 5,
        out_specs=VMEM,
        compiler_params=GRANT,
        cost_estimate=estimate(2),
    )(keep, got, bias, cosine, sine)


def attend_kernel(count, offset, table, query, *refs):
    sources = refs[:count]
    out, pairs, even, odd, high, weight, mixture = refs[count:]
    rows = sources[0].shape[0]
    lanes = query.shape[1]
    shard = table[0]
    factor = HEAD_DIM ** (-0.5) * LOG2E

    needed = jnp.int32(0)
    for slot in range(1, count):
        seen = table[offset + slot] < shard

        @pl.when(seen)
        def _(slot=slot, needed=needed):
            pairs[pl.ds(needed, 1)] = sources[slot][...][None]

        needed = needed + seen.astype(jnp.int32)

    def keys_of(at, size):
        return pairs[pl.ds(at, size), :, :HEAD_DIM].reshape(size * rows, HEAD_DIM)

    def values_of(at, size):
        return pairs[pl.ds(at, size), :, HEAD_DIM:].reshape(size * rows, HEAD_DIM).T

    def update(scores, values, fresh):
        top = jnp.max(scores, axis=0, keepdims=True)
        if not fresh:
            top = jnp.maximum(top, high[...])
        probs = jnp.exp2((scores - top) * factor)
        added = jnp.sum(probs, axis=0, keepdims=True)
        mixed = dot(values, probs.astype(jnp.bfloat16))
        if not fresh:
            scale = jnp.exp2((high[...] - top) * factor)
            added = added + weight[...] * scale
            mixed = mixed + mixture[...] * scale
        high[...] = top
        weight[...] = added
        mixture[...] = mixed

    scores = dot(sources[0][:, :HEAD_DIM], query[...])
    row = lax.broadcasted_iota(jnp.int32, scores.shape, 0)
    lane = lax.rem(lax.broadcasted_iota(jnp.int32, (1, lanes), 1), rows)
    update(jnp.where(row <= lane, scores, -jnp.inf), sources[0][:, HEAD_DIM:].T, True)

    single = lax.rem(needed, 2)

    @pl.when(single == 1)
    def _():
        update(dot(keys_of(0, 1), query[...]), values_of(0, 1), False)

    begin = single
    turns = needed // 2

    def step(turn, here, there):
        at = begin + 2 * jnp.minimum(turn + 1, turns - 1)
        there[...] = dot(keys_of(at, 2), query[...])
        update(here[...], values_of(begin + 2 * turn, 2), False)

    @pl.when(turns > 0)
    def _():
        even[...] = dot(keys_of(begin, 2), query[...])

        @pl.loop(0, (turns + 1) // 2)
        def _(index):
            step(2 * index, even, odd)

            @pl.when(2 * index + 1 < turns)
            def _():
                step(2 * index + 1, odd, even)

    value = (mixture[...] / weight[...]).T
    for head in range(lanes // rows):
        out[:, head * HEAD_DIM : (head + 1) * HEAD_DIM] = value[
            head * rows : (head + 1) * rows
        ].astype(jnp.bfloat16)


def attend(table, query, sources, offset):
    count = len(sources)
    lanes = query.shape[1]
    rows = sources[0].shape[0]
    shape = (rows, lanes // rows * HEAD_DIM)
    return pl.pallas_call(
        functools.partial(attend_kernel, count, offset),
        out_shape=jax.ShapeDtypeStruct(shape, jnp.bfloat16),
        in_specs=[SMEM, VMEM] + [VMEM] * count,
        out_specs=VMEM,
        scratch_shapes=[
            pltpu.VMEM((count, rows, 2 * HEAD_DIM), jnp.bfloat16),
            pltpu.VMEM((2 * rows, lanes), jnp.float32),
            pltpu.VMEM((2 * rows, lanes), jnp.float32),
            pltpu.VMEM((1, lanes), jnp.float32),
            pltpu.VMEM((1, lanes), jnp.float32),
            pltpu.VMEM((HEAD_DIM, lanes), jnp.float32),
        ],
        compiler_params=GRANT,
        cost_estimate=estimate(8),
    )(table, query, *sources)


def out_kernel(pieces, groups, share, place, *refs):
    weights = refs[4 * groups : 4 * groups + pieces]
    targets, source = refs[4 * groups + pieces : -1], refs[-1]
    rows, width = refs[0].shape[0] // 2, refs[0].shape[1]
    depth = width * groups
    near = pl.ds(pl.multiple_of(place[0] * rows, 16), rows)
    far = pl.ds(pl.multiple_of((1 - place[0]) * rows, 16), rows)
    for side in range(2):
        for index in range(groups):
            own, other = refs[side * groups + index], refs[(2 + side) * groups + index]
            columns = slice(index * width, (index + 1) * width)
            for part, (ref, span) in enumerate(
                ((own, near), (other, near), (own, far), (other, far))[: 2 * share]
            ):
                source[side, part * rows : (part + 1) * rows, columns] = ref[span, :]
    for piece in range(pieces):
        block = weights[piece]
        one = dot(source[0], block[:depth]).astype(jnp.bfloat16)
        two = dot(source[1], block[depth:]).astype(jnp.bfloat16)
        value = (one.astype(jnp.float32) + two.astype(jnp.float32)).astype(jnp.bfloat16)
        for part, target in enumerate(targets):
            target[piece] = value[part * rows : (part + 1) * rows]


def project_out(place, attended, weights, share):
    pieces = len(weights)
    groups = len(attended) // 4
    rows, depth = attended[0].shape[0], weights[0].shape[0] // 2
    columns = weights[0].shape[1]
    shape = jax.ShapeDtypeStruct((pieces, rows // 2, columns), jnp.bfloat16)
    return pl.pallas_call(
        functools.partial(out_kernel, pieces, groups, share),
        out_shape=(shape,) * (2 * share),
        in_specs=[SMEM] + [VMEM] * (4 * groups + pieces),
        out_specs=(VMEM,) * (2 * share),
        scratch_shapes=[pltpu.VMEM((2, share * rows, depth), jnp.bfloat16)],
        compiler_params=GRANT,
        cost_estimate=estimate(3),
    )(place, *attended, *weights)


def place_kernel(start, slots, width, table, place, *refs):
    keep, got, other, across = refs[:4]
    out, sems = refs[-2:]
    pieces, _, columns = keep.shape
    half = place[0]
    copies = []
    for piece in range(pieces):
        here = table[start + piece] * width
        there = table[slots + start + piece] * width
        for index, (value, base, side) in enumerate(
            (
                (keep, here, half),
                (got, here, 1 - half),
                (other, there, half),
                (across, there, 1 - half),
            )
        ):
            at = pl.multiple_of(base + side * columns, columns)
            copies.append(
                pltpu.make_async_copy(
                    value.at[piece], out.at[:, pl.ds(at, columns)], sems.at[index, piece]
                )
            )
    for copy in copies:
        copy.start()
    for copy in copies:
        copy.wait()


def place_part(table, place, parts, start, slots, width, whole):
    pieces, rows, columns = parts[0].shape
    extra = [] if whole is None else [whole]
    return pl.pallas_call(
        functools.partial(place_kernel, start, slots, width),
        out_shape=jax.ShapeDtypeStruct((rows, 4 * slots * columns), jnp.bfloat16),
        in_specs=[SMEM, SMEM] + [VMEM] * 4 + [HBM] * len(extra),
        out_specs=HBM,
        scratch_shapes=[pltpu.SemaphoreType.DMA((4, pieces))],
        input_output_aliases={6: 0} if extra else {},
        compiler_params=GRANT,
        cost_estimate=estimate(1),
    )(table, place, *parts, *extra)


def fast(
    seq_size, hidden, norm_gain, w_query, w_key, w_value, bias_query, bias_key,
    bias_value, w_out,
):
    rows, width = hidden.shape
    depth = w_query.shape[0]
    slots = seq_size // 2
    groups = 2
    shard = lax.axis_index("seq")
    side = lax.axis_index("head")
    table = jnp.stack(slot_shards(seq_size, shard) + slot_shards(seq_size, shard, -1))
    place = jnp.reshape(side, (1,)).astype(jnp.int32)

    q_first = pass_on(w_query, seq_size, 1)
    w_query_other = swap_core(w_query, seq_size)
    q_second = pass_on(w_query_other, seq_size, 1)
    q_weights = []
    for first, second in zip(halves(q_first, groups), halves(q_second, groups)):
        ring = ring_gather(first, second, seq_size, begin=2)
        q_weights.append([w_query, q_first, q_second] + ring[2:])
    w_kv = join(w_key, w_value)
    w_kv_other = swap_core(w_kv, seq_size)
    kv_weights = ring_gather(w_kv, w_kv_other, seq_size)
    mine, for_other = norm(table, hidden, norm_gain.reshape(1, width), slots, depth)

    positions = shard * rows + jnp.arange(rows, dtype=jnp.int32)
    half_dim = HEAD_DIM // 2
    freq = ROPE_BASE ** (-2.0 * jnp.arange(half_dim, dtype=jnp.float32) / HEAD_DIM)
    angles = positions.astype(jnp.float32)[:, None] * freq[None, :]
    cosine = jnp.cos(angles)
    sine = jnp.sin(angles)
    cosine = jnp.concatenate([cosine, cosine], axis=1)
    sine = jnp.concatenate([-sine, sine], axis=1)
    bias_kv = jnp.concatenate([bias_key, bias_value]).astype(jnp.float32)[None]
    bias_query = bias_query.astype(jnp.float32)[None]
    for_other, cosine, sine, bias_kv, bias_query = lax.optimization_barrier(
        (for_other, cosine, sine, bias_kv, bias_query)
    )
    other = swap_core(for_other, seq_size)

    keep, send = project(mine, other, kv_weights, 2 * HEAD_DIM, 0, 0, ())
    got = swap_core(send, seq_size)
    own_kv = keys_values(keep, got, bias_kv, cosine, sine)
    other_kv = swap_core(own_kv, seq_size)
    held = ring_gather(own_kv, other_kv, seq_size, -1)
    tokens = held + [other_kv]
    for one in held[1:]:
        tokens.append(swap_core(one, seq_size))

    columns = w_query.shape[1] // groups
    attended = []
    for index, weights in enumerate(q_weights):
        sums = ()
        start = 0
        for count in (slots - 3, 3):
            sums = project(
                mine, other, weights[start : start + count], columns, index, start,
                sums,
            )
            start += count
        keep, send = sums
        got = swap_core(send, seq_size)
        bias = bias_query[:, index * columns : (index + 1) * columns]
        query = queries(keep, got, bias, cosine, sine)
        attended.append(attend(table, query, tokens, 2 * slots))

    w_out_across = swap_head(w_out)
    piece, rest = cut(place, w_out, w_out_across)
    piece_other = swap_core(piece, seq_size)
    out_weights = ring_gather(piece, piece_other, seq_size)

    across, attended_other, across_other = [], [], []
    for one in attended:
        across.append(swap_head(one))
        attended_other.append(swap_core(one, seq_size))
        across_other.append(swap_core(across[-1], seq_size))
    operands = attended + across + attended_other + across_other
    keep, keep_other = project_out(place, operands, (piece, rest), 1)
    theirs = swap_core(keep_other, seq_size)
    own_parts = (keep[:1], keep[1:], theirs[:1], theirs[1:])
    whole = None
    start = 1
    for index, count in enumerate((slots - 6, 2, 2, 1)):
        keep, keep_other, send, send_other = project_out(
            place, operands, out_weights[start : start + count], 2
        )
        got = swap_head(send)
        got_other = swap_both(send_other, seq_size)
        kept_other = swap_core(keep_other, seq_size)
        whole = place_part(
            table, place, (keep, got, kept_other, got_other), start, slots,
            w_out.shape[1], whole,
        )
        if index == 0:
            whole = place_part(table, place, own_parts, 0, slots, w_out.shape[1], whole)
        start += count
    return whole


def rotary(values, positions):
    half_dim = values.shape[-1] // 2
    freq = ROPE_BASE ** (-2.0 * jnp.arange(half_dim, dtype=jnp.float32) / values.shape[-1])
    angles = positions.astype(jnp.float32)[:, None, None] * freq[None, None, :]
    cosine = jnp.cos(angles)
    sine = jnp.sin(angles)
    first = values[..., :half_dim]
    second = values[..., half_dim:]
    return jnp.concatenate(
        [first * cosine - second * sine, second * cosine + first * sine], axis=-1
    )


def plain(hidden, norm_gain, w_query, w_key, w_value, bias_query, bias_key, bias_value, w_out):
    rows = hidden.shape[0]
    heads = w_query.shape[1] // HEAD_DIM
    positions = lax.axis_index("seq") * rows + jnp.arange(rows, dtype=jnp.int32)
    widened = hidden.astype(jnp.float32)
    inverse = lax.rsqrt(jnp.mean(widened * widened, axis=-1, keepdims=True) + EPSILON)
    normed = (widened * inverse * norm_gain.astype(jnp.float32)).astype(jnp.bfloat16)
    weights = jnp.concatenate([w_query, w_key, w_value], axis=1)
    biases = jnp.concatenate([bias_query, bias_key, bias_value]).astype(jnp.float32)
    weights = lax.all_gather(weights, "seq", axis=0, tiled=True)
    qkv = jnp.dot(normed, weights, preferred_element_type=jnp.float32) + biases
    query, keys, values = jnp.split(
        qkv, [heads * HEAD_DIM, (heads + 1) * HEAD_DIM], axis=1
    )
    query = rotary(query.reshape(rows, heads, HEAD_DIM), positions).astype(jnp.bfloat16)
    keys = rotary(keys.reshape(rows, 1, HEAD_DIM), positions).reshape(rows, HEAD_DIM)
    pair = jnp.concatenate([keys, values], axis=1).astype(jnp.bfloat16)
    pair = lax.all_gather(pair, "seq", axis=0, tiled=True)
    scores = jnp.einsum(
        "qhd,kd->hqk", query, pair[:, :HEAD_DIM], preferred_element_type=jnp.float32
    )
    allowed = positions[:, None] >= jnp.arange(pair.shape[0], dtype=jnp.int32)[None, :]
    scores = jnp.where(allowed[None], scores * HEAD_DIM ** (-0.5), -jnp.inf)
    probs = jnp.exp(scores - jnp.max(scores, axis=-1, keepdims=True))
    total = jnp.sum(probs, axis=-1, keepdims=True)
    mixed = jnp.einsum(
        "hqk,kd->hqd",
        probs.astype(jnp.bfloat16),
        pair[:, HEAD_DIM:],
        preferred_element_type=jnp.float32,
    )
    attended = (mixed / total).astype(jnp.bfloat16)
    attended = attended.transpose(1, 0, 2).reshape(rows, heads * HEAD_DIM)
    partial_out = jnp.dot(
        attended,
        lax.all_gather(w_out, "seq", axis=1, tiled=True),
        preferred_element_type=jnp.float32,
    )
    return lax.psum_scatter(
        partial_out.astype(jnp.bfloat16), "head", scatter_dimension=0, tiled=True
    )


def local(seq_size, head_size, *args):
    hidden, w_query, w_out = args[0], args[2], args[8]
    fits = (
        head_size == 2
        and seq_size % 4 == 0
        and seq_size >= 8
        and hidden.shape[0] % 32 == 0
        and w_query.shape[0] % 128 == 0
        and w_out.shape[1] % 256 == 0
    )
    if fits:
        return fast(seq_size, *args)
    return plain(*args)


def solution(mesh):
    in_specs = (
        P("seq", None),
        P(),
        P("seq", "head"),
        P("seq", "head"),
        P("seq", "head"),
        P("head"),
        P("head"),
        P("head"),
        P("head", "seq"),
    )
    out_specs = P(("seq", "head"), None)
    body = functools.partial(local, mesh.shape["seq"], mesh.shape["head"])
    return jax.shard_map(
        body, mesh=mesh, in_specs=in_specs, out_specs=out_specs, check_vma=False
    )
```
